32 devices in a mesh: grp: 2 (over x), tok: 8 (over z, y), side: 2 (over core).
Axes of the slice: x: 2, y: 2, z: 4, core: 2. Of those that a mesh axis runs over, the one named last changes fastest.
Arguments:
- hidden_in: bfloat16 [512, 3072], P(('grp', 'tok')), parts along dimension 0, may hold values from -6 to 6
- queries: bfloat16 [512, 24, 128], P(('grp', 'tok'), 'side'), parts along dimension 0, may hold values from -32 to 32
- key_new: bfloat16 [512, 4, 128], P(('grp', 'tok'), 'side'), parts along dimension 0, may hold values from -32 to 32
- value_new: bfloat16 [512, 4, 128], P(('grp', 'tok'), 'side'), parts along dimension 0, may hold values from -6 to 6
- cache_keys: bfloat16 [512, 4, 128, 128], P(('grp', 'tok'), 'side'), parts along dimension 0, may hold values from -32 to 32
- cache_values: bfloat16 [512, 4, 128, 128], P(('grp', 'tok'), 'side'), parts along dimension 0, may hold values from -6 to 6
- lengths: int32 [512], P(('grp', 'tok')), parts along dimension 0, may hold values from 1 to 128, 16384 in all
- out_weight: bfloat16 [3072, 3072], P('side', 'tok'), may hold values from -0.109375 to 0.109375
- norm_gain: float32 [3072], replicated, may hold values from 0.1 to 1.9
- router_weight: float32 [3072, 4], replicated, may hold values from -0.109375 to 0.109375
- gate_weight: bfloat16 [3072, 32768], P(None, ('tok', 'side')), may hold values from -0.109375 to 0.109375
- up_weight: bfloat16 [3072, 32768], P(None, ('tok', 'side')), may hold values from -0.109375 to 0.109375
- down_weight: bfloat16 [32768, 3072], P(('tok', 'side')), may hold values from -0.0625 to 0.0625
- routes: int32 [512, 2], P('grp'), parts along dimension 0, may hold values from 0 to 3, all different within a row; in each aligned block of 32 rows (0 to 31, 32 to 63, ...) at most 24 rows name the same one
Outputs:
- mixed: bfloat16 [512, 3072], P(('grp', 'tok')), parts along dimension 0
The draws below stay inside these ranges and needn't reach their ends.
There are 2 independent parts, one for each index of `grp`. The reference program is written for one: setup_inputs(seed, part) draws one part's arguments, and reference() takes and returns one part's arrays. A program takes and returns all parts, laid end to end along the dimension named above; an argument that names none is the same for every part. Nothing has to cross between parts.
Inputs may be any that keep to these rules, and one draw needn't show every extreme that they name: Every sequence has at least one valid cache position and some sequence has 128; in each serving group the lengths sum to 16384. `routes`: each row names two different experts; among the rows of one index of tok (aligned blocks of 32 rows) no expert is named by more than 24 rows, and some expert reaches 24 in some block.
All inputs are finite; a program needn't handle non-finite values.
Results may differ from the reference program's by a relative error of at most 0.0075.
Values may be sent and summed in bfloat16 or wider, within the bound.
A program may use at most 128 MiB of HBM per device.

```python
import math
import jax
import jax.numpy as jnp
import numpy as np
from jax import lax

D = 3072
HEADS = 24
KV_HEADS = 4
HD = 128
EXPERTS = 4
HID = 8192
TOP = 2
SEQ_DEV = 32
L_MAX = 128
CAP = 24
SEQS = 256


def draw_queries(key, part):
    sampled = jnp.clip(jax.random.normal(jax.random.fold_in(key, 11), (SEQS, HEADS, HD), jnp.float32), -6.0, 6.0)
    return sampled.astype(jnp.bfloat16)


def draw_key_new(key, part):
    sampled = jnp.clip(jax.random.normal(jax.random.fold_in(key, 23), (SEQS, KV_HEADS, HD), jnp.float32), -6.0, 6.0)
    return sampled.astype(jnp.bfloat16)


def draw_cache_keys(key, part):
    sampled = jnp.clip(jax.random.normal(jax.random.fold_in(key, 37), (SEQS, KV_HEADS, L_MAX, HD), jnp.float32), -6.0, 6.0)
    return sampled.astype(jnp.bfloat16)


def steps_of(own_key, extent, pieces, least, top_value):
    factor_of, own = 1.0, jax.random.fold_in(own_key, 6)
    for dim, parts in pieces:
        heights = jnp.exp(jax.random.uniform(jax.random.fold_in(own, dim), (parts,), jnp.float32, least / len(pieces), top_value / len(pieces)))
        factor_of = factor_of * jnp.repeat(heights, extent[dim] // parts).reshape([-1 if axis == dim else 1 for axis in range(len(extent))])
    return factor_of


def profile(number_of, total, limit, slope):
    weights = [(1 << 20) // math.isqrt(standing ** slope) + 1 for standing in range(2, number_of + 1)]
    rest, counts = total - limit - (number_of - 1), [1] * (number_of - 1)
    while rest > 0:
        candidates = [i for i in range(number_of - 1) if counts[i] < limit]
        pool, budget = sum([weights[i] for i in candidates]), rest
        for i in candidates:
            extra = min(limit - counts[i], max(1, budget * weights[i] // pool), rest)
            counts[i] = counts[i] + extra
            rest = rest - extra
    return np.array([limit] + counts)


def ragged_sizes(own_key, number_of, total, most, skew):
    if number_of == 2:
        one = jax.random.randint(own_key, (), max(1, total - most), min(most, total - 1) + 1)
        return jnp.stack([one, total - one])
    sizes = jnp.asarray(profile(number_of, total, most, skew), jnp.int32)
    pairs = (number_of - 1) // 2
    source_of, taker = sizes[1:1 + 2 * pairs:2], sizes[2:2 + 2 * pairs:2]
    room = jnp.minimum(source_of - 1, most - taker)
    passed = jax.random.randint(jax.random.fold_in(own_key, 1), (pairs,), 0, 1 << 20) % (room + 1)
    sizes = sizes.at[1:1 + 2 * pairs:2].set(source_of - passed).at[2:2 + 2 * pairs:2].set(taker + passed)
    return sizes[jax.random.permutation(jax.random.fold_in(own_key, 2), number_of)]


def shared_out(own_key, own, number, rows, amount, top, bound, skew):
    ranking = jax.random.permutation(own_key, amount)
    heavy_load, usual = portions_of(amount, rows * top, bound, skew, True), portions_of(amount, rows * top, bound, skew, False)
    places = jnp.arange(amount)

    def named(sizes, turn):
        used = int((sizes > 0).sum())
        fixed = max(1, used // 4)
        moved = fixed + (places - fixed + turn * (used - fixed)) % max(1, amount - fixed)
        return jnp.zeros((amount,), jnp.int32).at[ranking[jnp.where(places < fixed, places, moved)]].set(jnp.asarray(sizes, jnp.int32))

    sizes = jnp.where(number % 4 == 0, named(heavy_load, number // 4), named(usual, number - number // 4 - 1))
    mixed = jax.random.permutation(jax.random.fold_in(own, 3), amount)
    source_of, sink = mixed[0:amount // 2 * 2:2], mixed[1:amount // 2 * 2:2]
    slack = jnp.minimum(sizes[source_of] - 1, bound - sizes[sink]) // 2
    slack = jnp.where((source_of == ranking[0]) | (sink == ranking[0]) | (sizes[sink] == 0), 0, jnp.maximum(slack, 0))
    moved = jax.random.randint(jax.random.fold_in(own, 4), (amount // 2,), 0, 1 << 20) % (slack + 1)
    sizes = sizes.at[source_of].add(-moved).at[sink].add(moved)
    labels = jnp.searchsorted(jnp.cumsum(sizes), jnp.arange(rows * top), side="right").astype(jnp.int32)
    table = labels.reshape(top, rows).T
    table = table[jax.random.permutation(jax.random.fold_in(own, 1), rows)]
    turn = jax.random.randint(jax.random.fold_in(own, 2), (rows, 1), 0, top)
    return jnp.take_along_axis(table, (jnp.arange(top)[None, :] + turn) % top, axis=1)


def portions_of(number_of, total, bound, slope, full):
    portions = [(1 << 20) // math.isqrt(standing ** slope) + 1 for standing in range(1, number_of + 1)]
    largest = bound if full else min(bound, max(-(-total // number_of), total * portions[0] // sum(portions)))
    least = 1 if total - largest >= number_of - 1 else 0
    counts, surplus = [largest] + [least] * (number_of - 1), total - largest - least * (number_of - 1)
    while surplus > 0:
        movable = [i for i in range(1, number_of) if counts[i] < largest] or [i for i in range(1, number_of) if counts[i] < bound]
        whole, budget = sum([portions[i] for i in movable]), surplus
        for i in movable:
            extra = min(bound - counts[i], max(1, budget * portions[i] // whole), surplus)
            counts[i] = counts[i] + extra
            surplus = surplus - extra
    return np.array(counts)


def noise(own_key, shape, scale, limit, cuts=(), kind=jnp.bfloat16):
    array = jax.random.normal(own_key, shape, jnp.float32) * scale
    if len(cuts) > 0:
        array = steps_of(own_key, shape, cuts, -0.22, 0.18) * array
    return jnp.clip(array, min=-limit, max=limit).astype(kind)


def setup_inputs(seed: int = 0, part: int = 0) -> dict:
    key_of = jax.random.split(jax.random.key(seed), 15)
    part_keys = jax.random.split(jax.random.fold_in(key_of[14], part), 15)
    hidden_in = noise(part_keys[0], (SEQS, D), 1.0, 6.0, ((0, 8),))
    queries = draw_queries(jax.random.fold_in(jax.random.fold_in(key_of[14], part), 71), part)
    key_new = draw_key_new(jax.random.fold_in(jax.random.fold_in(key_of[14], part), 71), part)
    value_new = noise(part_keys[3], (SEQS, KV_HEADS, HD), 1.0, 6.0, ((0, 8), (1, 2)))
    cache_keys = draw_cache_keys(jax.random.fold_in(jax.random.fold_in(key_of[14], part), 71), part)
    cache_values = noise(part_keys[5], (SEQS, KV_HEADS, L_MAX, HD), 1.0, 6.0, ((0, 8), (1, 2)))
    lengths = ragged_sizes(part_keys[6], SEQS, SEQS * L_MAX // 2, L_MAX, 2).astype(jnp.int32)
    out_weight = noise(key_of[7], (HEADS * HD, D), (HEADS * HD) ** -0.5, 0.109375, ((0, 2), (1, 8)))
    norm_gain = jnp.clip(1.0 + 0.18 * jax.random.normal(key_of[8], (D,), jnp.float32), 0.1, 1.9)
    router_weight = noise(key_of[9], (D, EXPERTS), D ** -0.5, 0.109375, (), jnp.float32)
    gate_weight = noise(key_of[10], (D, EXPERTS * HID), D ** -0.5, 0.109375, ((1, 16),))
    up_weight = noise(key_of[11], (D, EXPERTS * HID), D ** -0.5, 0.109375, ((1, 16),))
    down_weight = noise(key_of[12], (EXPERTS * HID, D), HID ** -0.5, 0.0625, ((0, 16),))
    routes_keys = jax.random.split(jax.random.fold_in(part_keys[13], 1), SEQS // SEQ_DEV)
    routes_turns = jax.random.permutation(jax.random.fold_in(part_keys[13], 3), SEQS // SEQ_DEV)
    routes = jax.vmap(lambda own, number: shared_out(jax.random.fold_in(part_keys[13], 2), own, number, SEQ_DEV, EXPERTS, TOP, CAP, 2))(routes_keys, routes_turns).reshape((SEQS, TOP))
    return dict(hidden_in=hidden_in, queries=queries, key_new=key_new, value_new=value_new, cache_keys=cache_keys, cache_values=cache_values, lengths=lengths, out_weight=out_weight, norm_gain=norm_gain, router_weight=router_weight, gate_weight=gate_weight, up_weight=up_weight, down_weight=down_weight, routes=routes)


def reference(hidden_in, queries, key_new, value_new, cache_keys, cache_values, lengths, out_weight, norm_gain, router_weight, gate_weight, up_weight, down_weight, routes):
    group_size = HEADS // KV_HEADS
    scaling = 1.0 / math.sqrt(HD)
    grouped = queries.astype(jnp.float32).reshape(SEQS, KV_HEADS, group_size, HD)
    scores = jnp.einsum('skgd,skpd->skgp', grouped, cache_keys.astype(jnp.float32)) * scaling
    usable = jnp.arange(L_MAX, dtype=jnp.int32)[None, :] < lengths[:, None]
    scores = jnp.where(usable[:, None, None, :], scores, -jnp.inf)
    own_score = jnp.einsum('skgd,skd->skg', grouped, key_new.astype(jnp.float32)) * scaling
    top_score = jnp.maximum(lax.optimization_barrier(jnp.max(scores, axis=-1)), own_score)
    weights = jnp.exp(scores - top_score[..., None])
    own_weight = jnp.exp(own_score - top_score)
    totals = lax.optimization_barrier(jnp.sum(weights, axis=-1)) + own_weight
    prob_low = (weights / totals[..., None]).astype(jnp.bfloat16)
    own_low = (own_weight / totals).astype(jnp.bfloat16)
    mixture = jnp.einsum('skgp,skpd->skgd', prob_low.astype(jnp.float32), cache_values.astype(jnp.float32))
    mixture = mixture + own_low.astype(jnp.float32)[..., None] * value_new.astype(jnp.float32)[:, :, None, :]
    attn_out = mixture.astype(jnp.bfloat16).reshape(SEQS, HEADS * HD)
    projected = jnp.dot(attn_out, out_weight, preferred_element_type=jnp.float32)
    residual = (hidden_in.astype(jnp.float32) + projected).astype(jnp.bfloat16)
    stream = residual.astype(jnp.float32)
    normed = (stream * lax.rsqrt(lax.optimization_barrier(jnp.mean(stream * stream, axis=-1, keepdims=True)) + 1e-05) * norm_gain).astype(jnp.bfloat16)
    logits = jnp.dot(normed.astype(jnp.float32), router_weight, precision=lax.Precision.HIGHEST)
    expert_ids = jnp.arange(EXPERTS, dtype=jnp.int32)
    picks = (routes[:, :, None] == expert_ids[None, None, :]).astype(jnp.float32)
    chosen_logits = lax.optimization_barrier(jnp.sum(picks * logits[:, None, :], axis=-1))
    leading = jax.nn.sigmoid(chosen_logits[:, 0] - chosen_logits[:, 1])
    gates = jnp.stack([leading, 1.0 - leading], axis=1)
    coefficient = lax.optimization_barrier(jnp.sum(gates[:, :, None] * picks, axis=1))

    def one_expert(index):
        gate_cols = lax.dynamic_slice_in_dim(gate_weight, index * HID, HID, 1)
        up_cols = lax.dynamic_slice_in_dim(up_weight, index * HID, HID, 1)
        down_rows = lax.dynamic_slice_in_dim(down_weight, index * HID, HID, 0)
        gated = jnp.dot(normed, gate_cols, preferred_element_type=jnp.float32)
        upward = jnp.dot(normed, up_cols, preferred_element_type=jnp.float32)
        active = (jax.nn.silu(gated) * upward).astype(jnp.bfloat16)
        return jnp.dot(active, down_rows, preferred_element_type=jnp.float32)
    outputs = lax.map(one_expert, expert_ids)
    combined = lax.optimization_barrier(jnp.sum(coefficient.T[:, :, None] * outputs, axis=0))
    return (stream + combined).astype(jnp.bfloat16)
```

```python
import functools
import math

import jax
import jax.numpy as jnp
from jax import lax
from jax.experimental import pallas as pl
from jax.experimental.pallas import tpu as pltpu
from jax.sharding import PartitionSpec as P

CAP = 24
HIDDEN_TILE = 512
STRIPS = 3
GROUP = 16
CHUNK = 8

bf, f32, i32 = jnp.bfloat16, jnp.float32, jnp.int32


def wire(block):
    rows, width = block.shape
    half = width // 2
    tail = jnp.concatenate([block[16:, :half], block[16:, half:]], axis=0)
    return jnp.concatenate([block[:16], tail], axis=1).astype(bf)


def unwire(block, width):
    half = width // 2
    full = block.astype(f32)
    tail = jnp.concatenate([full[:8, width:], full[8:, width:]], axis=1)
    return jnp.concatenate([full[:, :width], tail], axis=0)


def aligned(start, step):
    return pl.multiple_of(start, step)


def body(
    dims,
    lengths_ref,
    q_ref,
    kn_ref,
    vn_ref,
    hidden_ref,
    routes_t_ref,
    gain_ref,
    router_ref,
    k_hbm,
    v_hbm,
    out_hbm,
    gate_hbm,
    up_hbm,
    down_hbm,
    out_ref,
    k_buf,
    v_buf,
    heads,
    hid_out,
    hid_in,
    proj,
    peer,
    resw,
    place_s,
    rank_s,
    put_s,
    stage,
    X,
    first_s,
    other_s,
    rs_s,
    coef_s,
    resid,
    a_s,
    acc_g,
    acc_u,
    active,
    out_w,
    gate_w,
    up_w,
    down_w,
    mine,
    theirs,
    theirs_in,
    y_out,
    y_in,
    zt,
    z_out,
    z_in,
    final,
    kv_sem,
    w_sem,
    a_zs,
    a_ys,
    a_r,
    h_s,
    h_r,
    p_s,
    p_r,
    x_zs,
    x_ys,
    x_os,
    x_r,
    c_s,
    c_r,
    ry_s,
    ry_r,
    rz_s,
    rz_r,
    f_s,
    f_r,
):
    T, Z, R, rows, cap = dims
    ZH, RH = Z // 2, R // 2
    D = hidden_ref.shape[1]
    half_d = D // 2
    total = T * rows
    slots = T * cap
    part = Z * cap
    hid = gate_w.shape[1]
    width = out_w.shape[1]
    wide = R * width
    wave_rows = ZH * R * rows
    _, kv_count, places, head_width = k_buf.shape
    group = q_ref.shape[0] // kv_count
    pieces = (rows // GROUP) * kv_count
    piece_width = group * head_width
    tok = lax.axis_index("tok")
    side = lax.axis_index("side")
    z = tok // R
    r = tok % R
    other = 1 - side
    far = jnp.where(z < ZH, 1, -1)
    near_count = jnp.where(z < ZH, z, Z - 1 - z)

    def ro(d):
        return (r + d) % R

    def nearest(k):
        if k == 0:
            return z
        close = (k + 1) // 2
        close_way = -far if k % 2 == 1 else far
        return jnp.where(k <= 2 * near_count, z + close_way * close, z + far * (k - near_count))

    order = [nearest(k) for k in range(Z)]
    waves = [z // ZH, 1 - z // ZH]

    def copy(src, dst, ssem, rsem, t=None, s=None):
        where = {"tok": tok if t is None else t, "side": side if s is None else s}
        return pltpu.make_async_remote_copy(
            src_ref=src,
            dst_ref=dst,
            send_sem=ssem,
            recv_sem=rsem,
            device_id=where,
            device_id_type=pl.DeviceIdType.MESH,
        )

    pending = []

    def start(c, cond=None):
        pending.append((c, cond))
        if cond is None:
            c.start()
        else:
            pl.when(cond)(c.start)

    barrier = pltpu.get_barrier_semaphore()
    for d in range(1, T):
        pl.semaphore_signal(
            barrier,
            inc=1,
            device_id={"tok": (tok + d) % T, "side": side},
            device_id_type=pl.DeviceIdType.MESH,
        )
    pl.semaphore_signal(
        barrier, inc=1, device_id={"tok": tok, "side": other}, device_id_type=pl.DeviceIdType.MESH
    )

    def kv_load(piece):
        h, g = divmod(piece, kv_count)
        at = pl.ds(h * GROUP, GROUP)
        return [
            pltpu.make_async_copy(k_hbm.at[at, g], k_buf.at[at, g], kv_sem.at[0, piece]),
            pltpu.make_async_copy(v_hbm.at[at, g], v_buf.at[at, g], kv_sem.at[1, piece]),
        ]

    kv_loads = [kv_load(piece) for piece in range(pieces)]
    for pair in kv_loads:
        for load in pair:
            load.start()
    loads = [
        pltpu.make_async_copy(out_hbm, out_w, w_sem.at[0]),
        pltpu.make_async_copy(gate_hbm, gate_w, w_sem.at[1]),
        pltpu.make_async_copy(up_hbm, up_w, w_sem.at[2]),
        pltpu.make_async_copy(down_hbm, down_w, w_sem.at[3]),
    ]
    for load in loads:
        load.start()

    scaling = 1.0 / math.sqrt(head_width)
    eye = lax.broadcasted_iota(i32, (rows, rows), 0) == lax.broadcasted_iota(i32, (rows, rows), 1)
    lens = jnp.sum(jnp.where(eye, lengths_ref[...], 0), axis=1, keepdims=True)
    unit = group * CHUNK
    seq_of = lax.rem(lax.broadcasted_iota(i32, (unit, 1), 0), CHUNK)
    cols_at = lax.broadcasted_iota(i32, (unit, CHUNK * places), 1) - seq_of * places
    own_at = lax.broadcasted_iota(i32, (unit, rows * kv_count), 1) - seq_of * kv_count
    low = -1e30
    kn = kn_ref[...]
    vn = vn_ref[...]

    def attend(c, g):
        q = q_ref[g * group : (g + 1) * group, c * CHUNK : (c + 1) * CHUNK, :]
        q = q.astype(f32).reshape(unit, head_width).astype(bf)
        keys = k_buf[c * CHUNK : (c + 1) * CHUNK, g].reshape(CHUNK * places, head_width)
        vals = v_buf[c * CHUNK : (c + 1) * CHUNK, g].reshape(CHUNK * places, head_width)
        dn = (((1,), (1,)), ((), ()))
        s = lax.dot_general(q, keys, dn, preferred_element_type=f32) * scaling
        so = lax.dot_general(q, kn, dn, preferred_element_type=f32) * scaling
        size = jnp.concatenate([lens[c * CHUNK : (c + 1) * CHUNK]] * group, axis=0)
        s = jnp.where((cols_at >= 0) & (cols_at < size), s, low)
        so = jnp.where(own_at == c * CHUNK * kv_count + g, so, low)
        top = jnp.maximum(
            jnp.max(s, axis=1, keepdims=True), jnp.max(so, axis=1, keepdims=True)
        )
        w = jnp.exp(s - top)
        wo = jnp.exp(so - top)
        inv = 1.0 / (jnp.sum(w, axis=1, keepdims=True) + jnp.sum(wo, axis=1, keepdims=True))
        o = jnp.dot((w * inv).astype(bf), vals, preferred_element_type=f32)
        return o + jnp.dot((wo * inv).astype(bf), vn, preferred_element_type=f32)

    def slot1(t, piece):
        h, g = divmod(piece, kv_count)
        return heads.at[
            pl.ds(aligned(t * rows + h * GROUP, GROUP), GROUP),
            pl.ds(g * piece_width, piece_width),
        ]

    def along(zs, way, piece):
        here = slot1(zs * R + r, piece)
        c = copy(
            here,
            here,
            a_zs.at[(way + 1) // 2, zs, piece],
            a_r.at[zs * R + r, piece],
            t=lax.rem(z + way + Z, Z) * R + r,
        )
        start(c, (z + way >= 0) & (z + way < Z))

    def across(zs, piece):
        here = slot1(zs * R + r, piece)
        for e in range(1, R):
            start(
                copy(
                    here,
                    here,
                    a_ys.at[e, zs, piece],
                    a_r.at[zs * R + r, piece],
                    t=z * R + ro(e),
                )
            )

    def landed1(t, piece):
        here = slot1(t, piece)
        copy(here, here, a_r.at[t, piece], a_r.at[t, piece]).wait_recv()

    home = r // RH == side

    for piece in range(pieces):
        h, g = divmod(piece, kv_count)
        for load in kv_loads[piece]:
            load.wait()
        halves = [attend(c, g) for c in range(h * GROUP // CHUNK, (h + 1) * GROUP // CHUNK)]
        at = pl.ds(aligned(tok * rows + h * GROUP, GROUP), GROUP)
        for k in range(group):
            block = jnp.concatenate([o[k * CHUNK : (k + 1) * CHUNK] for o in halves], axis=0)
            col = (g * group + k) * head_width
            heads[at, col : col + head_width] = block.astype(bf)
        if piece == 0:
            pl.semaphore_wait(barrier, T)
        for way in (1, -1):
            along(z, way, piece)
        across(z, piece)

    for t in range(T):
        hid_out[t] = hidden_ref[:, t * width : (t + 1) * width]

    @pl.when(home)
    def _():
        hid_in[tok] = hid_out[tok]

    for d in range(1, T):
        t = (tok + d) % T
        start(copy(hid_out.at[t], hid_in.at[tok], h_s.at[d], h_r.at[tok], t=t), home)

    resw[...] = jnp.zeros_like(resw)
    lanes = lax.broadcasted_iota(i32, (1, total), 1)
    block_of = lax.div(lanes, rows)
    route0 = routes_t_ref[0:1, :]
    route1 = routes_t_ref[1:2, :]
    erow = lax.broadcasted_iota(i32, (8, total), 0)
    hit8 = (route0 == erow) | (route1 == erow)
    row_i = lax.broadcasted_iota(i32, (total, total), 0)
    col_i = lax.broadcasted_iota(i32, (total, total), 1)
    before = (row_i < col_i) & (lax.div(row_i, rows) == lax.div(col_i, rows))
    rank8 = jnp.dot(
        jnp.where(hit8, 1.0, 0.0).astype(bf),
        jnp.where(before, 1.0, 0.0).astype(bf),
        preferred_element_type=f32,
    ).astype(i32)
    rank_s[...] = rank8
    zs_of = lax.div(block_of, R)
    place_s[...] = jnp.where(hit8 & (rank8 < cap), lax.rem(zs_of, ZH) * cap + rank8, -1)
    wave_lane_r = lax.rem(
        lax.div(lax.broadcasted_iota(i32, (1, wave_rows), 1), rows), R
    )
    wave_row = lax.broadcasted_iota(i32, (ZH * cap, wave_rows), 0)
    for i, w in enumerate(waves):
        placed = place_s[:, pl.ds(aligned(w * wave_rows, wave_rows), wave_rows)]
        for j in range(RH):
            fits = wave_lane_r == side * RH + j
            for e in range(Z):
                want = jnp.where(fits, placed[e : e + 1], -1)
                put_s[i, j, e * ZH * cap : (e + 1) * ZH * cap, :] = jnp.where(
                    wave_row == want, 1.0, 0.0
                ).astype(bf)
    my_rank = rank_s[pl.ds(z, 1), :]
    my_hit = (route0 == z) | (route1 == z)
    target = jnp.where(
        my_hit & (my_rank < cap), (lax.rem(block_of, R) * Z + zs_of) * cap + my_rank, -1
    )
    code = (route0 + route1 - z).astype(f32) + jnp.where(route0 == z, 16.0, 0.0)
    codes = jnp.sum(
        jnp.where(lax.broadcasted_iota(i32, (slots, total), 0) == target, code, 0.0),
        axis=1,
        keepdims=True,
    )
    is_first = jnp.where(codes >= 16.0, 1.0, 0.0)
    first_s[...] = jnp.broadcast_to(is_first, first_s.shape)
    other_s[...] = jnp.broadcast_to((codes - 16.0 * is_first).astype(i32), other_s.shape)

    def xslot(t, rp, w):
        return X.at[t, rp, w]

    def x_across(zs, j, w):
        t, rp = zs * R + r, side * RH + j
        for e in range(1, R):
            start(
                copy(
                    xslot(t, rp, w),
                    xslot(t, rp, w),
                    x_ys.at[e, zs, j, w],
                    x_r.at[t, rp, w],
                    t=z * R + ro(e),
                )
            )

    def x_over(t, j, w):
        rp = side * RH + j
        start(
            copy(
                xslot(t, rp, w), xslot(t, rp, w), x_os.at[t, j, w], x_r.at[t, rp, w], s=other
            )
        )

    def x_landed(t, rp, w):
        copy(xslot(t, rp, w), xslot(t, rp, w), x_r.at[t, rp, w], x_r.at[t, rp, w]).wait_recv()

    def project(i):
        w = waves[i]
        p = jnp.dot(
            heads[pl.ds(aligned(w * wave_rows, wave_rows), wave_rows), :],
            out_w[...],
            preferred_element_type=f32,
        )
        proj[i] = p.reshape(ZH, 2, RH * rows, width)
        c = copy(proj.at[i, :, other], peer.at[i], p_s.at[i], p_r.at[i], s=other)
        start(c)
        for zl in range(ZH):
            for j in range(RH):
                b = (w * ZH + zl) * R + side * RH + j

                @pl.when(b != tok)
                def _(b=b):
                    copy(hid_in.at[b], hid_in.at[b], h_r.at[b], h_r.at[b]).wait_recv()

        c.wait_recv()
        for zl in range(ZH):
            b0 = (w * ZH + zl) * R + side * RH
            whole = (
                proj[i, zl, side]
                + peer[i, zl]
                + hid_in[pl.ds(b0, RH)].astype(f32).reshape(RH * rows, width)
            )
            resw[zl, pl.ds(side * RH, RH)] = whole.astype(bf).reshape(RH, rows, width)
        for j in range(RH):
            packed = jnp.dot(
                put_s[i, j],
                resw[...].reshape(wave_rows, width),
                preferred_element_type=f32,
            )
            stage[i, j] = packed.astype(bf).reshape(Z, ZH * cap, width)
            rp = side * RH + j
            X[tok, rp, w] = stage[i, j, z]
            x_across(z, j, w)
            for k in range(1, Z):
                zd = order[k]
                start(
                    copy(
                        stage.at[i, j, zd],
                        xslot(tok, rp, w),
                        x_zs.at[i, j, zd],
                        x_r.at[tok, rp, w],
                        t=zd * R + r,
                    )
                )
            x_over(tok, j, w)

    loads[0].wait()
    for k in range(1, Z):
        zs = order[k]
        way = jnp.where(zs < z, 1, -1)
        for piece in range(pieces):
            landed1(zs * R + r, piece)
            along(zs, way, piece)
            across(zs, piece)
        last = order[k - 1]
        for e in range(1, R):
            for piece in range(pieces):
                landed1(last * R + ro(e), piece)
        if k == ZH:
            project(0)
    for e in range(1, R):
        for piece in range(pieces):
            landed1(order[Z - 1] * R + ro(e), piece)
    project(1)

    loads[1].wait()
    loads[2].wait()
    tile = min(HIDDEN_TILE, hid)
    squares = jnp.zeros((slots, 1), f32)
    logits = jnp.zeros((slots, Z), f32)

    def spread(ref, n):
        return jnp.concatenate([ref[...]] * (n // 128), axis=1)

    def absorb(zs, idx, squares, logits):
        for r2 in range(R):
            for rp in range(RH):
                for w in range(2):
                    x_landed(zs * R + r2, other * RH + rp, w)
        x = jnp.concatenate(
            [X[zs * R + r2].reshape(slots, width) for r2 in range(R)], axis=1
        ).astype(f32)
        cols = pl.ds(aligned(zs * wide, wide), wide)
        squares = squares + jnp.sum(x * x, axis=1, keepdims=True)
        a = (x * gain_ref[:, cols]).astype(bf)
        a_s[...] = a
        resid[:, cols] = (x * spread(first_s, wide)).astype(bf)
        left = router_ref[:, cols]
        for _ in range(3):
            now = left.astype(bf)
            left = left - now.astype(f32)
            logits = logits + lax.dot_general(
                a, now, (((1,), (1,)), ((), ())), preferred_element_type=f32
            )
        if idx == Z - 1:
            rs = lax.rsqrt(squares / D + 1e-05)
            rs_s[...] = jnp.broadcast_to(rs, rs_s.shape)

        @pl.loop(0, hid // tile)
        def _(n):
            here = pl.ds(aligned(n * tile, tile), tile)
            g = jnp.dot(a_s[...], gate_w[cols, here], preferred_element_type=f32)
            u = jnp.dot(a_s[...], up_w[cols, here], preferred_element_type=f32)
            if idx > 0:
                g = acc_g[:, here] + g
                u = acc_u[:, here] + u
            if idx < Z - 1:
                acc_g[:, here] = g
                acc_u[:, here] = u
            else:
                scale = spread(rs_s, tile)
                g = g * scale
                u = u * scale
                active[:, here] = (g / (1.0 + jnp.exp(-g)) * u).astype(bf)

        return squares, logits

    for k in range(1, Z + 1):
        if k < Z:
            zs = order[k]
            lead = zs // ZH
            for w in (lead, 1 - lead):
                for j in range(RH):
                    x_landed(zs * R + r, side * RH + j, w)
                    x_across(zs, j, w)
                    x_over(zs * R + r, j, w)
        last = order[k - 1]
        lead = last // ZH
        for e in range(1, R):
            for w in (lead, 1 - lead):
                for j in range(RH):
                    x_landed(last * R + ro(e), side * RH + j, w)
                    x_over(last * R + ro(e), j, w)
        squares, logits = absorb(last, k - 1, squares, logits)

    logits = logits * rs_s[:, :1]
    elane = lax.broadcasted_iota(i32, (slots, Z), 1)
    l_self = jnp.sum(jnp.where(elane == z, logits, 0.0), axis=1, keepdims=True)
    l_other = jnp.sum(jnp.where(elane == other_s[:, :Z], logits, 0.0), axis=1, keepdims=True)
    coef_s[...] = jnp.broadcast_to(1.0 / (1.0 + jnp.exp(l_other - l_self)), coef_s.shape)

    loads[3].wait()
    strip = half_d // STRIPS
    own_part = pl.ds(aligned(r * part, part), part)

    def down(start_at, q):
        at = pl.ds(aligned(start_at * half_d + q * strip, 128), strip)
        return jnp.dot(active[...], down_w[:, at], preferred_element_type=f32)

    def y_copy(q, e):
        i = (q, e)
        return copy(y_out.at[i], y_in.at[i], ry_s.at[i], ry_r.at[i], t=z * R + ro(e))

    for q in range(STRIPS):
        theirs[q] = down(other, q).astype(bf)
        c = copy(theirs.at[q], theirs_in.at[q], c_s.at[q], c_r.at[q], s=other)
        start(c)
        mine[q] = down(side, q)
        c.wait_recv()
        mine[q] = (mine[q] + theirs_in[q].astype(f32)) * spread(coef_s, strip)
        for e in range(1, R):
            at = pl.ds(aligned(ro(e) * part, part), part)
            y_out[q, e] = mine[q, at, :].astype(bf)
            start(y_copy(q, e))

    lane_t = lax.broadcasted_iota(i32, (rows, total), 1)
    at_own = lane_t == tok * rows + lax.broadcasted_iota(i32, (rows, total), 0)
    r0 = jnp.sum(jnp.where(at_own, route0, 0), axis=1, keepdims=True)
    r1 = jnp.sum(jnp.where(at_own, route1, 0), axis=1, keepdims=True)
    lane = lax.broadcasted_iota(i32, (rows, 128), 1)
    both = jnp.where((lane == r0) | (lane == r1), 1.0, 0.0).astype(bf)
    row_n = lax.broadcasted_iota(i32, (rows, rows), 0)
    col_n = lax.broadcasted_iota(i32, (rows, rows), 1)
    ranks = jnp.dot(
        jnp.where(col_n < row_n, 1.0, 0.0).astype(bf), both, preferred_element_type=f32
    ).astype(i32)
    at_part = lax.broadcasted_iota(i32, (rows, part), 1)

    def find(k):
        rank = jnp.sum(jnp.where(lane == k, ranks, 0), axis=1, keepdims=True)
        return at_part == k * cap + rank

    pick = jnp.where(find(r0) | find(r1), 1.0, 0.0).astype(bf)

    for q in range(STRIPS):
        cols = pl.ds(aligned(side * half_d + q * strip, 128), strip)
        rows_sum = mine[q, own_part, :] + resid[own_part, cols].astype(f32)
        for e in range(1, R):
            y_copy(q, e).wait_recv()
            rows_sum = rows_sum + y_in[q, e].astype(f32)
        zt[...] = rows_sum
        for k in range(Z):
            to = jnp.where(z < ZH, Z - 1 - k, k)
            z_out[q, to] = wire(zt[pl.ds(aligned(to * cap, 8), cap), :])
            c = copy(
                z_out.at[q, to],
                z_in.at[q, z],
                rz_s.at[q, to],
                rz_r.at[q, z],
                t=to * R + r,
            )
            start(c, to != z)

            @pl.when(to == z)
            def _(q=q, to=to):
                z_in[q, z] = z_out[q, to]

    for q in range(STRIPS):
        for d in range(1, Z):
            src = lax.rem(z + d, Z)
            here = z_in.at[q, src]
            copy(here, here, rz_r.at[q, src], rz_r.at[q, src]).wait_recv()
        got = jnp.concatenate([unwire(z_in[q, e], strip) for e in range(Z)], axis=0)
        done = jnp.dot(pick, got.astype(bf), preferred_element_type=f32).astype(bf)
        final[side, q] = done
        here = final.at[side, q]
        start(copy(here, here, f_s.at[q], f_r.at[q], s=other))
    for q in range(STRIPS):
        there = final.at[other, q]
        copy(there, there, f_r.at[q], f_r.at[q]).wait_recv()
    for s in range(2):
        for q in range(STRIPS):
            out_ref[:, s * half_d + q * strip : s * half_d + (q + 1) * strip] = final[s, q]
    for c, cond in pending:
        if cond is None:
            c.wait_send()
        else:
            pl.when(cond)(c.wait_send)


def local(
    hidden_in,
    queries,
    key_new,
    value_new,
    cache_keys,
    cache_values,
    lengths,
    out_weight,
    norm_gain,
    router_weight,
    gate_weight,
    up_weight,
    down_weight,
    routes,
):
    rows, D = hidden_in.shape
    _, head_count, head_width = queries.shape
    kv_count = key_new.shape[1]
    T = lax.axis_size("tok")
    Z = router_weight.shape[1]
    R = T // Z
    ZH, RH = Z // 2, R // 2
    cap = min(CAP, rows)
    slots = T * cap
    part = Z * cap
    hid = gate_weight.shape[1]
    width = out_weight.shape[1]
    wave_rows = ZH * R * rows
    pieces = (rows // GROUP) * kv_count
    half_d = D // 2
    strip = half_d // STRIPS
    wire_width = strip * cap // 16
    dma = pltpu.SemaphoreType.DMA
    vmem = pl.BlockSpec(memory_space=pltpu.VMEM)
    anyspace = pl.BlockSpec(memory_space=pl.ANY)
    return pl.pallas_call(
        functools.partial(body, (T, Z, R, rows, cap)),
        out_shape=jax.ShapeDtypeStruct((rows, D), bf),
        in_specs=[vmem] * 8 + [anyspace] * 6,
        out_specs=vmem,
        scratch_shapes=[
            pltpu.VMEM(cache_keys.shape, bf),
            pltpu.VMEM(cache_values.shape, bf),
            pltpu.VMEM((T * rows, head_count * head_width), bf),
            pltpu.VMEM((T, rows, width), bf),
            pltpu.VMEM((T, rows, width), bf),
            pltpu.VMEM((2, ZH, 2, RH * rows, width), f32),
            pltpu.VMEM((2, ZH, RH * rows, width), f32),
            pltpu.VMEM((ZH, R, rows, width), bf),
            pltpu.VMEM((8, T * rows), i32),
            pltpu.VMEM((8, T * rows), i32),
            pltpu.VMEM((2, RH, Z * ZH * cap, wave_rows), bf),
            pltpu.VMEM((2, RH, Z, ZH * cap, width), bf),
            pltpu.VMEM((T, R, 2, ZH * cap, width), bf),
            pltpu.VMEM((slots, 128), f32),
            pltpu.VMEM((slots, 128), i32),
            pltpu.VMEM((slots, 128), f32),
            pltpu.VMEM((slots, 128), f32),
            pltpu.VMEM((slots, D), bf),
            pltpu.VMEM((slots, R * width), bf),
            pltpu.VMEM((slots, hid), f32),
            pltpu.VMEM((slots, hid), f32),
            pltpu.VMEM((slots, hid), bf),
            pltpu.VMEM(out_weight.shape, bf),
            pltpu.VMEM(gate_weight.shape, bf),
            pltpu.VMEM(up_weight.shape, bf),
            pltpu.VMEM(down_weight.shape, bf),
            pltpu.VMEM((STRIPS, slots, strip), f32),
            pltpu.VMEM((STRIPS, slots, strip), bf),
            pltpu.VMEM((STRIPS, slots, strip), bf),
            pltpu.VMEM((STRIPS, R, part, strip), bf),
            pltpu.VMEM((STRIPS, R, part, strip), bf),
            pltpu.VMEM((part, strip), f32),
            pltpu.VMEM((STRIPS, Z, 16, wire_width), bf),
            pltpu.VMEM((STRIPS, Z, 16, wire_width), bf),
            pltpu.VMEM((2, STRIPS, rows, strip), bf),
            dma((2, pieces)),
            dma((4,)),
            dma((2, Z, pieces)),
            dma((R, Z, pieces)),
            dma((T, pieces)),
            dma((T,)),
            dma((T,)),
            dma((2,)),
            dma((2,)),
            dma((2, RH, Z)),
            dma((R, Z, RH, 2)),
            dma((T, RH, 2)),
            dma((T, R, 2)),
            dma((STRIPS,)),
            dma((STRIPS,)),
            dma((STRIPS, R)),
            dma((STRIPS, R)),
            dma((STRIPS, Z)),
            dma((STRIPS, Z)),
            dma((STRIPS,)),
            dma((STRIPS,)),
        ],
        compiler_params=pltpu.CompilerParams(
            collective_id=0, has_side_effects=True, vmem_limit_bytes=67043328
        ),
    )(
        lengths.reshape(1, rows),
        jnp.transpose(queries, (1, 0, 2)),
        key_new.reshape(rows * kv_count, head_width),
        value_new.reshape(rows * kv_count, head_width),
        hidden_in,
        routes.T,
        norm_gain.reshape(1, D),
        router_weight.T,
        cache_keys,
        cache_values,
        out_weight,
        gate_weight,
        up_weight,
        down_weight,
    )


def solution(mesh):
    return jax.shard_map(
        local,
        mesh=mesh,
        in_specs=(
            P(("grp", "tok"), None),
            P(("grp", "tok"), "side", None),
            P(("grp", "tok"), "side", None),
            P(("grp", "tok"), "side", None),
            P(("grp", "tok"), "side", None, None),
            P(("grp", "tok"), "side", None, None),
            P(("grp", "tok")),
            P("side", "tok"),
            P(),
            P(),
            P(None, ("tok", "side")),
            P(None, ("tok", "side")),
            P(("tok", "side"), None),
            P("grp", None),
        ),
        out_specs=P(("grp", "tok"), None),
        check_vma=False,
    )
```

```python
import functools
import math

import jax
import jax.numpy as jnp
from jax import lax
from jax.experimental import pallas as pl
from jax.experimental.pallas import tpu as pltpu
from jax.sharding import PartitionSpec as P

CAP = 24
HIDDEN_TILE = 512
STRIPS = 3
GROUP = 16
CHUNK = 8

bf, f32, i32 = jnp.bfloat16, jnp.float32, jnp.int32


def wire(block):
    rows, width = block.shape
    half = width // 2
    tail = jnp.concatenate([block[16:, :half], block[16:, half:]], axis=0)
    return jnp.concatenate([block[:16], tail], axis=1).astype(bf)


def unwire(block, width):
    half = width // 2
    full = block.astype(f32)
    tail = jnp.concatenate([full[:8, width:], full[8:, width:]], axis=1)
    return jnp.concatenate([full[:, :width], tail], axis=0)


def aligned(start, step):
    return pl.multiple_of(start, step)


def body(
    dims,
    lengths_ref,
    q_ref,
    kn_ref,
    vn_ref,
    hidden_ref,
    routes_t_ref,
    gain_ref,
    router_ref,
    k_hbm,
    v_hbm,
    out_hbm,
    gate_hbm,
    up_hbm,
    down_hbm,
    out_ref,
    k_buf,
    v_buf,
    heads,
    hid_out,
    hid_in,
    proj,
    peer,
    resw,
    place_s,
    rank_s,
    put_s,
    stage,
    X,
    first_s,
    other_s,
    rs_s,
    coef_s,
    resid,
    a_s,
    acc_g,
    acc_u,
    active,
    out_w,
    gate_w,
    up_w,
    down_w,
    mine,
    theirs,
    theirs_in,
    y_out,
    y_in,
    z_out,
    z_in,
    final,
    kv_sem,
    w_sem,
    hello,
    a_zs,
    a_ys,
    a_r,
    h_s,
    h_r,
    p_s,
    p_r,
    x_zs,
    x_ys,
    x_os,
    x_r,
    c_s,
    c_r,
    ry_s,
    ry_r,
    rz_s,
    rz_r,
    f_s,
    f_r,
):
    T, Z, R, rows, cap = dims
    ZH, RH = Z // 2, R // 2
    D = hidden_ref.shape[1]
    half_d = D // 2
    total = T * rows
    slots = T * cap
    part = Z * cap
    hid = gate_w.shape[1]
    width = out_w.shape[1]
    wide = R * width
    wave_rows = ZH * R * rows
    _, kv_count, places, head_width = k_buf.shape
    group = q_ref.shape[0] // kv_count
    pieces = (rows // GROUP) * kv_count
    piece_width = group * head_width
    tok = lax.axis_index("tok")
    side = lax.axis_index("side")
    z = tok // R
    r = tok % R
    other = 1 - side
    def ro(d):
        return (r + d) % R

    order = [jnp.where(k <= z, z - k, k) for k in range(Z)]
    waves = [0, 1]

    def copy(src, dst, ssem, rsem, t=None, s=None):
        where = {"tok": tok if t is None else t, "side": side if s is None else s}
        return pltpu.make_async_remote_copy(
            src_ref=src,
            dst_ref=dst,
            send_sem=ssem,
            recv_sem=rsem,
            device_id=where,
            device_id_type=pl.DeviceIdType.MESH,
        )

    pending = []

    def start(c, cond=None):
        pending.append((c, cond))
        if cond is None:
            c.start()
        else:
            pl.when(cond)(c.start)

    barrier = pltpu.get_barrier_semaphore()

    def greet(t, s):
        pl.semaphore_signal(
            barrier,
            inc=1,
            device_id={"tok": t, "side": s},
            device_id_type=pl.DeviceIdType.MESH,
        )

    @pl.when(z > 0)
    def _():
        greet(tok - R, side)

    @pl.when(z < Z - 1)
    def _():
        greet(tok + R, side)

    for e in range(1, R):
        greet(z * R + ro(e), side)
    greet(tok, other)
    neighbours = R + jnp.where(z > 0, 1, 0) + jnp.where(z < Z - 1, 1, 0)

    def kv_load(piece):
        h, g = divmod(piece, kv_count)
        at = pl.ds(h * GROUP, GROUP)
        return [
            pltpu.make_async_copy(k_hbm.at[at, g], k_buf.at[at, g], kv_sem.at[0, piece]),
            pltpu.make_async_copy(v_hbm.at[at, g], v_buf.at[at, g], kv_sem.at[1, piece]),
        ]

    kv_loads = [kv_load(piece) for piece in range(pieces)]
    for pair in kv_loads:
        for load in pair:
            load.start()
    loads = [
        pltpu.make_async_copy(out_hbm, out_w, w_sem.at[0]),
        pltpu.make_async_copy(gate_hbm, gate_w, w_sem.at[1]),
        pltpu.make_async_copy(up_hbm, up_w, w_sem.at[2]),
        pltpu.make_async_copy(down_hbm, down_w, w_sem.at[3]),
    ]

    scaling = 1.0 / math.sqrt(head_width)
    eye = lax.broadcasted_iota(i32, (rows, rows), 0) == lax.broadcasted_iota(i32, (rows, rows), 1)
    lens = jnp.sum(jnp.where(eye, lengths_ref[...], 0), axis=1, keepdims=True)
    unit = group * CHUNK
    seq_of = lax.rem(lax.broadcasted_iota(i32, (unit, 1), 0), CHUNK)
    cols_at = lax.broadcasted_iota(i32, (unit, CHUNK * places), 1) - seq_of * places
    own_at = lax.broadcasted_iota(i32, (unit, rows * kv_count), 1) - seq_of * kv_count
    low = -1e30
    kn = kn_ref[...]
    vn = vn_ref[...]

    def attend(c, g):
        q = q_ref[g * group : (g + 1) * group, c * CHUNK : (c + 1) * CHUNK, :]
        q = q.astype(f32).reshape(unit, head_width).astype(bf)
        keys = k_buf[c * CHUNK : (c + 1) * CHUNK, g].reshape(CHUNK * places, head_width)
        vals = v_buf[c * CHUNK : (c + 1) * CHUNK, g].reshape(CHUNK * places, head_width)
        dn = (((1,), (1,)), ((), ()))
        s = lax.dot_general(q, keys, dn, preferred_element_type=f32) * scaling
        so = lax.dot_general(q, kn, dn, preferred_element_type=f32) * scaling
        size = jnp.concatenate([lens[c * CHUNK : (c + 1) * CHUNK]] * group, axis=0)
        s = jnp.where((cols_at >= 0) & (cols_at < size), s, low)
        so = jnp.where(own_at == c * CHUNK * kv_count + g, so, low)
        top = jnp.maximum(
            jnp.max(s, axis=1, keepdims=True), jnp.max(so, axis=1, keepdims=True)
        )
        w = jnp.exp(s - top)
        wo = jnp.exp(so - top)
        inv = 1.0 / (jnp.sum(w, axis=1, keepdims=True) + jnp.sum(wo, axis=1, keepdims=True))
        o = jnp.dot((w * inv).astype(bf), vals, preferred_element_type=f32)
        return o + jnp.dot((wo * inv).astype(bf), vn, preferred_element_type=f32)

    def slot1(t, piece):
        h, g = divmod(piece, kv_count)
        return heads.at[
            pl.ds(aligned(t * rows + h * GROUP, GROUP), GROUP),
            pl.ds(g * piece_width, piece_width),
        ]

    def along(to, piece, cond):
        here = slot1(tok, piece)
        to = lax.rem(to + Z, Z)
        start(copy(here, here, a_zs.at[to, piece], a_r.at[tok, piece], t=to * R + r), cond)

    def tell(way):
        pl.semaphore_signal(
            hello.at[(1 - way) // 2],
            inc=1,
            device_id={"tok": tok + way * R, "side": side},
            device_id_type=pl.DeviceIdType.MESH,
        )

    def reach(n):
        for way in (1, -1):
            to = z + way * (n + 1)

            @pl.when((to >= 0) & (to < Z))
            def _(way=way):
                pl.semaphore_wait(hello.at[(1 + way) // 2], 1)

                @pl.when((z - way >= 0) & (z - way < Z))
                def _():
                    tell(-way)

            for piece in range(pieces):
                along(to, piece, (to >= 0) & (to < Z))

    def across(zs, piece):
        here = slot1(zs * R + r, piece)
        for e in range(1, R):
            start(
                copy(
                    here,
                    here,
                    a_ys.at[e, zs, piece],
                    a_r.at[zs * R + r, piece],
                    t=z * R + ro(e),
                )
            )

    def landed1(t, piece):
        here = slot1(t, piece)
        copy(here, here, a_r.at[t, piece], a_r.at[t, piece]).wait_recv()

    home = r // RH == side

    for piece in range(pieces):
        h, g = divmod(piece, kv_count)
        for load in kv_loads[piece]:
            load.wait()
        if piece == pieces - 1:
            for load in loads:
                load.start()
        halves = [attend(c, g) for c in range(h * GROUP // CHUNK, (h + 1) * GROUP // CHUNK)]
        at = pl.ds(aligned(tok * rows + h * GROUP, GROUP), GROUP)
        for k in range(group):
            block = jnp.concatenate([o[k * CHUNK : (k + 1) * CHUNK] for o in halves], axis=0)
            col = (g * group + k) * head_width
            heads[at, col : col + head_width] = block.astype(bf)
        if piece == 0:
            pl.semaphore_wait(barrier, neighbours)
            inner = (z > 0) & (z < Z - 1)
            for way in (1, -1):
                pl.when(inner)(functools.partial(tell, way))
        for way in (1, -1):
            along(z + way, piece, (z + way >= 0) & (z + way < Z))
        across(z, piece)

    if Z > 2:
        reach(1)

    for t in range(T):
        hid_out[t] = hidden_ref[:, t * width : (t + 1) * width]

    @pl.when(home)
    def _():
        hid_in[tok] = hid_out[tok]

    def lend(t):
        start(copy(hid_out.at[t], hid_in.at[tok], h_s.at[t], h_r.at[tok], t=t), home)

    for e in range(1, R):
        lend(z * R + ro(e))

    resw[...] = jnp.zeros_like(resw)
    lanes = lax.broadcasted_iota(i32, (1, total), 1)
    block_of = lax.div(lanes, rows)
    route0 = routes_t_ref[0:1, :]
    route1 = routes_t_ref[1:2, :]
    erow = lax.broadcasted_iota(i32, (8, total), 0)
    hit8 = (route0 == erow) | (route1 == erow)
    row_i = lax.broadcasted_iota(i32, (total, total), 0)
    col_i = lax.broadcasted_iota(i32, (total, total), 1)
    before = (row_i < col_i) & (lax.div(row_i, rows) == lax.div(col_i, rows))
    rank8 = jnp.dot(
        jnp.where(hit8, 1.0, 0.0).astype(bf),
        jnp.where(before, 1.0, 0.0).astype(bf),
        preferred_element_type=f32,
    ).astype(i32)
    rank_s[...] = rank8
    zs_of = lax.div(block_of, R)
    place_s[...] = jnp.where(hit8 & (rank8 < cap), lax.rem(zs_of, ZH) * cap + rank8, -1)
    wave_lane_r = lax.rem(
        lax.div(lax.broadcasted_iota(i32, (1, wave_rows), 1), rows), R
    )
    wave_row = lax.broadcasted_iota(i32, (ZH * cap, wave_rows), 0)
    for i, w in enumerate(waves):
        placed = place_s[:, pl.ds(aligned(w * wave_rows, wave_rows), wave_rows)]
        for j in range(RH):
            fits = wave_lane_r == side * RH + j
            for e in range(Z):
                want = jnp.where(fits, placed[e : e + 1], -1)
                put_s[i, j, e * ZH * cap : (e + 1) * ZH * cap, :] = jnp.where(
                    wave_row == want, 1.0, 0.0
                ).astype(bf)
    my_rank = rank_s[pl.ds(z, 1), :]
    my_hit = (route0 == z) | (route1 == z)
    target = jnp.where(
        my_hit & (my_rank < cap),
        (lax.rem(block_of, R) * Z + zs_of) * cap + my_rank,
        -1,
    )
    code = (route0 + route1 - z).astype(f32) + jnp.where(route0 == z, 16.0, 0.0)
    codes = jnp.sum(
        jnp.where(lax.broadcasted_iota(i32, (slots, total), 0) == target, code, 0.0),
        axis=1,
        keepdims=True,
    )
    is_first = jnp.where(codes >= 16.0, 1.0, 0.0)
    first_s[...] = jnp.broadcast_to(is_first, first_s.shape)
    other_s[...] = jnp.broadcast_to((codes - 16.0 * is_first).astype(i32), other_s.shape)

    def xslot(t, rp, w):
        return X.at[t, rp, w]

    def x_across(zs, j, w):
        t, rp = zs * R + r, side * RH + j
        for e in range(1, R):
            start(
                copy(
                    xslot(t, rp, w),
                    xslot(t, rp, w),
                    x_ys.at[e, zs, j, w],
                    x_r.at[t, rp, w],
                    t=z * R + ro(e),
                )
            )

    def x_over(t, j, w):
        rp = side * RH + j
        start(
            copy(
                xslot(t, rp, w), xslot(t, rp, w), x_os.at[t, j, w], x_r.at[t, rp, w], s=other
            )
        )

    def x_landed(t, rp, w):
        copy(xslot(t, rp, w), xslot(t, rp, w), x_r.at[t, rp, w], x_r.at[t, rp, w]).wait_recv()

    def project(i):
        w = waves[i]
        p = jnp.dot(
            heads[pl.ds(aligned(w * wave_rows, wave_rows), wave_rows), :],
            out_w[...],
            preferred_element_type=f32,
        )
        proj[i] = p.reshape(ZH, 2, RH * rows, width)
        c = copy(proj.at[i, :, other], peer.at[i], p_s.at[i], p_r.at[i], s=other)
        start(c)
        for zl in range(ZH):
            for j in range(RH):
                b = (w * ZH + zl) * R + side * RH + j

                @pl.when(b != tok)
                def _(b=b):
                    copy(hid_in.at[b], hid_in.at[b], h_r.at[b], h_r.at[b]).wait_recv()

        c.wait_recv()
        for zl in range(ZH):
            b0 = (w * ZH + zl) * R + side * RH
            whole = (
                proj[i, zl, side]
                + peer[i, zl]
                + hid_in[pl.ds(b0, RH)].astype(f32).reshape(RH * rows, width)
            )
            resw[zl, pl.ds(side * RH, RH)] = whole.astype(bf).reshape(RH, rows, width)
        for j in range(RH):
            packed = jnp.dot(
                put_s[i, j],
                resw[...].reshape(wave_rows, width),
                preferred_element_type=f32,
            )
            stage[i, j] = packed.astype(bf).reshape(Z, ZH * cap, width)
            rp = side * RH + j
            X[tok, rp, w] = stage[i, j, z]
            x_across(z, j, w)
            x_over(tok, j, w)
        for k in range(1, Z):
            deliver(i, k)

    def deliver(i, k):
        zd, w = order[k], waves[i]
        for j in range(RH):
            rp = side * RH + j
            start(
                copy(
                    stage.at[i, j, zd],
                    xslot(tok, rp, w),
                    x_zs.at[i, j, zd],
                    x_r.at[tok, rp, w],
                    t=zd * R + r,
                )
            )

    def relay_z(w, k):
        zs = order[k]
        for j in range(RH):
            x_landed(zs * R + r, side * RH + j, w)
            x_across(zs, j, w)
            x_over(zs * R + r, j, w)

    def relay_y(w, k):
        zs = order[k]
        for e in range(1, R):
            for j in range(RH):
                x_landed(zs * R + ro(e), side * RH + j, w)
                x_over(zs * R + ro(e), j, w)

    loads[0].wait()

    def crossed(zs):
        for e in range(1, R):
            for piece in range(pieces):
                landed1(zs * R + ro(e), piece)

    for k in range(1, Z):
        zs = order[k]
        for piece in range(pieces):
            landed1(zs * R + r, piece)
            across(zs, piece)
            if piece == 0:
                lend(zs * R + r)
                for e in range(1, R):
                    lend(zs * R + ro(e))
        if k < Z - 2:
            reach(k + 1)
    for w in range(2):
        for zs in range(w * ZH, (w + 1) * ZH):
            crossed(zs)
        project(w)
    for k in range(1, Z):
        relay_z(0, k)
    for k in range(Z):
        relay_y(0, k)

    tile = min(HIDDEN_TILE, hid)
    strip = half_d // STRIPS

    def spread(block, n):
        return jnp.concatenate([block] * (n // 128), axis=1)

    def absorb(zs, idx, squares, logits):
        for r2 in range(R):
            for rp in range(RH):
                for w in range(2):
                    x_landed(zs * R + r2, other * RH + rp, w)
        x = jnp.concatenate(
            [X[zs * R + r2].reshape(slots, width) for r2 in range(R)], axis=1
        ).astype(f32)
        cols = pl.ds(aligned(zs * wide, wide), wide)
        squares = squares + jnp.sum(x * x, axis=1, keepdims=True)
        a = (x * gain_ref[:, cols]).astype(bf)
        a_s[...] = a
        resid[:, cols] = (x * spread(first_s[...], wide)).astype(bf)
        left = router_ref[:, cols]
        for _ in range(3):
            now = left.astype(bf)
            left = left - now.astype(f32)
            logits = logits + lax.dot_general(
                a, now, (((1,), (1,)), ((), ())), preferred_element_type=f32
            )
        if idx == Z - 1:
            rs = lax.rsqrt(squares / D + 1e-05)
            rs_s[...] = jnp.broadcast_to(rs, rs_s.shape)

        @pl.loop(0, hid // tile)
        def _(n):
            here = pl.ds(aligned(n * tile, tile), tile)
            g = jnp.dot(a_s[...], gate_w[cols, here], preferred_element_type=f32)
            u = jnp.dot(a_s[...], up_w[cols, here], preferred_element_type=f32)
            if idx > 0:
                g = acc_g[:, here] + g
                u = acc_u[:, here] + u
            if idx < Z - 1:
                acc_g[:, here] = g
                acc_u[:, here] = u
            else:
                scale = spread(rs_s[...], tile)
                g = g * scale
                u = u * scale
                active[:, here] = (g / (1.0 + jnp.exp(-g)) * u).astype(bf)

        return squares, logits

    def down(which, q):
        at = pl.ds(aligned(which * half_d + q * strip, 128), strip)
        return jnp.dot(active[...], down_w[:, at], preferred_element_type=f32)

    def y_copy(q, e):
        i = (q, e)
        return copy(y_out.at[i], y_in.at[i], ry_s.at[i], ry_r.at[i], t=z * R + ro(e))

    swaps = []

    def contract(q):
        theirs[q] = down(other, q).astype(bf)
        c = copy(theirs.at[q], theirs_in.at[q], c_s.at[q], c_r.at[q], s=other)
        start(c)
        swaps.append(c)
        mine[q] = down(side, q)

    def pass_on(q):
        swaps[q].wait_recv()
        mine[q] = (mine[q] + theirs_in[q].astype(f32)) * spread(coef_s[...], strip)
        for e in range(1, R):
            at = pl.ds(aligned(ro(e) * part, part), part)
            y_out[q, e] = mine[q, at, :].astype(bf)
            start(y_copy(q, e))

    def send_back(q):
        own = pl.ds(aligned(r * part, part), part)
        cols = pl.ds(aligned(side * half_d + q * strip, 128), strip)
        rows_sum = mine[q, own, :] + resid[own, cols].astype(f32)
        for e in range(1, R):
            y_copy(q, e).wait_recv()
            rows_sum = rows_sum + y_in[q, e].astype(f32)
        for to in range(Z):
            z_out[q, to] = wire(rows_sum[to * cap : (to + 1) * cap])
            c = copy(
                z_out.at[q, to], z_in.at[q, z], rz_s.at[q, to], rz_r.at[q, z], t=to * R + r
            )
            start(c, z != to)

            @pl.when(z == to)
            def _(q=q, to=to):
                z_in[q, z] = z_out[q, to]

    squares, logits = jnp.zeros((slots, 1), f32), jnp.zeros((slots, Z), f32)
    relay_z(1, 1)
    relay_y(1, 0)
    for k in range(Z):
        if k + 2 < Z:
            relay_z(1, k + 2)
        if k + 1 < Z:
            relay_y(1, k + 1)
        if k == 0:
            loads[1].wait()
            loads[2].wait()
        squares, logits = absorb(order[k], k, squares, logits)
    logits = logits * rs_s[:, :1]
    elane = lax.broadcasted_iota(i32, (slots, Z), 1)
    l_self = jnp.sum(jnp.where(elane == z, logits, 0.0), axis=1, keepdims=True)
    l_other = jnp.sum(jnp.where(elane == other_s[:, :Z], logits, 0.0), axis=1, keepdims=True)
    coef_s[...] = jnp.broadcast_to(1.0 / (1.0 + jnp.exp(l_other - l_self)), coef_s.shape)
    loads[3].wait()
    for q in range(STRIPS):
        contract(q)
        if q > 0:
            pass_on(q - 1)
    pass_on(STRIPS - 1)

    lane_t = lax.broadcasted_iota(i32, (rows, total), 1)
    at_own = lane_t == tok * rows + lax.broadcasted_iota(i32, (rows, total), 0)
    r0 = jnp.sum(jnp.where(at_own, route0, 0), axis=1, keepdims=True)
    r1 = jnp.sum(jnp.where(at_own, route1, 0), axis=1, keepdims=True)
    lane = lax.broadcasted_iota(i32, (rows, 128), 1)
    both = jnp.where((lane == r0) | (lane == r1), 1.0, 0.0).astype(bf)
    row_n = lax.broadcasted_iota(i32, (rows, rows), 0)
    col_n = lax.broadcasted_iota(i32, (rows, rows), 1)
    ranks = jnp.dot(
        jnp.where(col_n < row_n, 1.0, 0.0).astype(bf), both, preferred_element_type=f32
    ).astype(i32)
    at_part = lax.broadcasted_iota(i32, (rows, part), 1)

    def find(k):
        rank = jnp.sum(jnp.where(lane == k, ranks, 0), axis=1, keepdims=True)
        return at_part == k * cap + rank

    pick = jnp.where(find(r0) | find(r1), 1.0, 0.0).astype(bf)

    for q in range(STRIPS):
        send_back(q)
    for q in range(STRIPS):
        for d in range(1, Z):
            src = lax.rem(z + d, Z)
            here = z_in.at[q, src]
            copy(here, here, rz_r.at[q, src], rz_r.at[q, src]).wait_recv()
        got = jnp.concatenate([unwire(z_in[q, e], strip) for e in range(Z)], axis=0)
        done = jnp.dot(pick, got.astype(bf), preferred_element_type=f32).astype(bf)
        final[side, q] = done
        here = final.at[side, q]
        start(copy(here, here, f_s.at[q], f_r.at[q], s=other))
    for q in range(STRIPS):
        there = final.at[other, q]
        copy(there, there, f_r.at[q], f_r.at[q]).wait_recv()
    for s in range(2):
        for q in range(STRIPS):
            out_ref[:, s * half_d + q * strip : s * half_d + (q + 1) * strip] = final[s, q]
    for c, cond in pending:
        if cond is None:
            c.wait_send()
        else:
            pl.when(cond)(c.wait_send)


def local(
    hidden_in,
    queries,
    key_new,
    value_new,
    cache_keys,
    cache_values,
    lengths,
    out_weight,
    norm_gain,
    router_weight,
    gate_weight,
    up_weight,
    down_weight,
    routes,
):
    rows, D = hidden_in.shape
    _, head_count, head_width = queries.shape
    kv_count = key_new.shape[1]
    T = lax.axis_size("tok")
    Z = router_weight.shape[1]
    R = T // Z
    ZH, RH = Z // 2, R // 2
    cap = min(CAP, rows)
    slots = T * cap
    part = Z * cap
    hid = gate_weight.shape[1]
    width = out_weight.shape[1]
    wave_rows = ZH * R * rows
    pieces = (rows // GROUP) * kv_count
    half_d = D // 2
    strip = half_d // STRIPS
    wire_width = strip * cap // 16
    dma = pltpu.SemaphoreType.DMA
    vmem = pl.BlockSpec(memory_space=pltpu.VMEM)
    anyspace = pl.BlockSpec(memory_space=pl.ANY)
    return pl.pallas_call(
        functools.partial(body, (T, Z, R, rows, cap)),
        out_shape=jax.ShapeDtypeStruct((rows, D), bf),
        in_specs=[vmem] * 8 + [anyspace] * 6,
        out_specs=vmem,
        scratch_shapes=[
            pltpu.VMEM(cache_keys.shape, bf),
            pltpu.VMEM(cache_values.shape, bf),
            pltpu.VMEM((T * rows, head_count * head_width), bf),
            pltpu.VMEM((T, rows, width), bf),
            pltpu.VMEM((T, rows, width), bf),
            pltpu.VMEM((2, ZH, 2, RH * rows, width), f32),
            pltpu.VMEM((2, ZH, RH * rows, width), f32),
            pltpu.VMEM((ZH, R, rows, width), bf),
            pltpu.VMEM((8, T * rows), i32),
            pltpu.VMEM((8, T * rows), i32),
            pltpu.VMEM((2, RH, Z * ZH * cap, wave_rows), bf),
            pltpu.VMEM((2, RH, Z, ZH * cap, width), bf),
            pltpu.VMEM((T, R, 2, ZH * cap, width), bf),
            pltpu.VMEM((slots, 128), f32),
            pltpu.VMEM((slots, 128), i32),
            pltpu.VMEM((slots, 128), f32),
            pltpu.VMEM((slots, 128), f32),
            pltpu.VMEM((slots, D), bf),
            pltpu.VMEM((slots, R * width), bf),
            pltpu.VMEM((slots, hid), f32),
            pltpu.VMEM((slots, hid), f32),
            pltpu.VMEM((slots, hid), bf),
            pltpu.VMEM(out_weight.shape, bf),
            pltpu.VMEM(gate_weight.shape, bf),
            pltpu.VMEM(up_weight.shape, bf),
            pltpu.VMEM(down_weight.shape, bf),
            pltpu.VMEM((STRIPS, slots, strip), f32),
            pltpu.VMEM((STRIPS, slots, strip), bf),
            pltpu.VMEM((STRIPS, slots, strip), bf),
            pltpu.VMEM((STRIPS, R, part, strip), bf),
            pltpu.VMEM((STRIPS, R, part, strip), bf),
            pltpu.VMEM((STRIPS, Z, 16, wire_width), bf),
            pltpu.VMEM((STRIPS, Z, 16, wire_width), bf),
            pltpu.VMEM((2, STRIPS, rows, strip), bf),
            dma((2, pieces)),
            dma((4,)),
            pltpu.SemaphoreType.REGULAR((2,)),
            dma((Z, pieces)),
            dma((R, Z, pieces)),
            dma((T, pieces)),
            dma((T,)),
            dma((T,)),
            dma((2,)),
            dma((2,)),
            dma((2, RH, Z)),
            dma((R, Z, RH, 2)),
            dma((T, RH, 2)),
            dma((T, R, 2)),
            dma((STRIPS,)),
            dma((STRIPS,)),
            dma((STRIPS, R)),
            dma((STRIPS, R)),
            dma((STRIPS, Z)),
            dma((STRIPS, Z)),
            dma((STRIPS,)),
            dma((STRIPS,)),
        ],
        compiler_params=pltpu.CompilerParams(
            collective_id=0, has_side_effects=True, vmem_limit_bytes=67043328
        ),
    )(
        lengths.reshape(1, rows),
        jnp.transpose(queries, (1, 0, 2)),
        key_new.reshape(rows * kv_count, head_width),
        value_new.reshape(rows * kv_count, head_width),
        hidden_in,
        routes.T,
        norm_gain.reshape(1, D),
        router_weight.T,
        cache_keys,
        cache_values,
        out_weight,
        gate_weight,
        up_weight,
        down_weight,
    )


def solution(mesh):
    return jax.shard_map(
        local,
        mesh=mesh,
        in_specs=(
            P(("grp", "tok"), None),
            P(("grp", "tok"), "side", None),
            P(("grp", "tok"), "side", None),
            P(("grp", "tok"), "side", None),
            P(("grp", "tok"), "side", None, None),
            P(("grp", "tok"), "side", None, None),
            P(("grp", "tok")),
            P("side", "tok"),
            P(),
            P(),
            P(None, ("tok", "side")),
            P(None, ("tok", "side")),
            P(("tok", "side"), None),
            P("grp", None),
        ),
        out_specs=P(("grp", "tok"), None),
        check_vma=False,
    )
```

```python
import functools
import math

import jax
import jax.numpy as jnp
from jax import lax
from jax.experimental import pallas as pl
from jax.experimental.pallas import tpu as pltpu
from jax.sharding import PartitionSpec as P

CAP = 24
HIDDEN_TILE = 2048
STRIPS = 3
GROUP = 16
CHUNK = 8

bf, f32, i32 = jnp.bfloat16, jnp.float32, jnp.int32


def wire(block):
    rows, width = block.shape
    half = width // 2
    tail = jnp.concatenate([block[16:, :half], block[16:, half:]], axis=0)
    return jnp.concatenate([block[:16], tail], axis=1).astype(bf)


def unwire(block, width):
    half = width // 2
    full = block.astype(f32)
    tail = jnp.concatenate([full[:8, width:], full[8:, width:]], axis=1)
    return jnp.concatenate([full[:, :width], tail], axis=0)


def aligned(start, step):
    return pl.multiple_of(start, step)


def body(
    dims,
    lengths_hbm,
    q_hbm,
    kn_hbm,
    vn_hbm,
    hidden_hbm,
    routes_t_hbm,
    gain_hbm,
    router_hbm,
    k_hbm,
    v_hbm,
    out_hbm,
    gate_hbm,
    up_hbm,
    down_hbm,
    out_ref,
    lengths_ref,
    q_ref,
    kn_ref,
    vn_ref,
    hidden_ref,
    routes_t_ref,
    gain_ref,
    router_ref,
    small_sem,
    k_buf,
    v_buf,
    heads,
    hid_out,
    hid_in,
    proj,
    peer,
    resw,
    place_s,
    rank_s,
    put_s,
    stage,
    X,
    first_s,
    other_s,
    rs_s,
    coef_s,
    resid,
    a_s,
    acc_g,
    acc_u,
    active,
    out_w,
    gate_w,
    up_w,
    down_w,
    mine,
    theirs,
    theirs_in,
    y_out,
    y_in,
    z_out,
    z_in,
    kv_sem,
    w_sem,
    hello,
    a_zs,
    a_fs,
    a_ys,
    a_r,
    h_s,
    h_r,
    p_s,
    p_r,
    x_zs,
    x_ys,
    x_os,
    x_r,
    c_s,
    c_r,
    ry_s,
    ry_r,
    rz_s,
    rz_r,
    f_s,
    f_r,
):
    T, Z, R, rows, cap = dims
    ZH, RH = Z // 2, R // 2
    D = hidden_ref.shape[1]
    half_d = D // 2
    total = T * rows
    slots = T * cap
    part = Z * cap
    hid = gate_w.shape[1]
    width = out_w.shape[1]
    wide = R * width
    wave_rows = ZH * R * rows
    _, kv_count, places, head_width = k_buf.shape
    group = q_ref.shape[0] // kv_count
    pieces = (rows // GROUP) * kv_count
    piece_width = group * head_width
    tok = lax.axis_index("tok")
    side = lax.axis_index("side")
    z = tok // R
    r = tok % R
    other = 1 - side
    def ro(d):
        return (r + d) % R

    order = [jnp.where(k <= z, z - k, k) for k in range(Z)]
    waves = [0, 1]

    def copy(src, dst, ssem, rsem, t=None, s=None):
        where = {"tok": tok if t is None else t, "side": side if s is None else s}
        return pltpu.make_async_remote_copy(
            src_ref=src,
            dst_ref=dst,
            send_sem=ssem,
            recv_sem=rsem,
            device_id=where,
            device_id_type=pl.DeviceIdType.MESH,
        )

    pending = []

    def start(c, cond=None):
        pending.append((c, cond))
        if cond is None:
            c.start()
        else:
            pl.when(cond)(c.start)

    barrier = pltpu.get_barrier_semaphore()

    def greet(t, s):
        pl.semaphore_signal(
            barrier,
            inc=1,
            device_id={"tok": t, "side": s},
            device_id_type=pl.DeviceIdType.MESH,
        )

    @pl.when(z > 0)
    def _():
        greet(tok - R, side)

    @pl.when(z < Z - 1)
    def _():
        greet(tok + R, side)

    for e in range(1, R):
        greet(z * R + ro(e), side)
    greet(tok, other)
    neighbours = R + jnp.where(z > 0, 1, 0) + jnp.where(z < Z - 1, 1, 0)

    def kv_load(piece):
        h, g = divmod(piece, kv_count)
        at = pl.ds(h * GROUP, GROUP)
        return [
            pltpu.make_async_copy(k_hbm.at[at, g], k_buf.at[at, g], kv_sem.at[0, piece]),
            pltpu.make_async_copy(v_hbm.at[at, g], v_buf.at[at, g], kv_sem.at[1, piece]),
        ]

    smalls = [
        pltpu.make_async_copy(src, dst, small_sem.at[i])
        for i, (src, dst) in enumerate(
            (
                (lengths_hbm, lengths_ref),
                (q_hbm, q_ref),
                (kn_hbm, kn_ref),
                (vn_hbm, vn_ref),
                (hidden_hbm, hidden_ref),
                (routes_t_hbm, routes_t_ref),
                (gain_hbm, gain_ref),
                (router_hbm, router_ref),
            )
        )
    ]
    for load in smalls[:4]:
        load.start()
    kv_loads = [kv_load(piece) for piece in range(pieces)]
    for pair in kv_loads:
        for load in pair:
            load.start()
    for load in smalls[4:]:
        load.start()
    for load in smalls[:4]:
        load.wait()
    loads = [
        pltpu.make_async_copy(out_hbm, out_w, w_sem.at[0]),
        pltpu.make_async_copy(gate_hbm, gate_w, w_sem.at[1]),
        pltpu.make_async_copy(up_hbm, up_w, w_sem.at[2]),
        pltpu.make_async_copy(down_hbm, down_w, w_sem.at[3]),
    ]

    scaling = 1.0 / math.sqrt(head_width)
    eye = lax.broadcasted_iota(i32, (rows, rows), 0) == lax.broadcasted_iota(i32, (rows, rows), 1)
    lens = jnp.sum(jnp.where(eye, lengths_ref[...], 0), axis=1, keepdims=True)
    unit = group * CHUNK
    seq_of = lax.rem(lax.broadcasted_iota(i32, (unit, 1), 0), CHUNK)
    cols_at = lax.broadcasted_iota(i32, (unit, CHUNK * places), 1) - seq_of * places
    own_at = lax.broadcasted_iota(i32, (unit, rows * kv_count), 1) - seq_of * kv_count
    low = -1e30
    kn = kn_ref[...]
    vn = vn_ref[...]

    def attend(c, g):
        q = q_ref[g * group : (g + 1) * group, c * CHUNK : (c + 1) * CHUNK, :]
        q = q.astype(f32).reshape(unit, head_width).astype(bf)
        keys = k_buf[c * CHUNK : (c + 1) * CHUNK, g].reshape(CHUNK * places, head_width)
        vals = v_buf[c * CHUNK : (c + 1) * CHUNK, g].reshape(CHUNK * places, head_width)
        dn = (((1,), (1,)), ((), ()))
        s = lax.dot_general(q, keys, dn, preferred_element_type=f32) * scaling
        so = lax.dot_general(q, kn, dn, preferred_element_type=f32) * scaling
        size = jnp.concatenate([lens[c * CHUNK : (c + 1) * CHUNK]] * group, axis=0)
        s = jnp.where((cols_at >= 0) & (cols_at < size), s, low)
        so = jnp.where(own_at == c * CHUNK * kv_count + g, so, low)
        top = jnp.maximum(
            jnp.max(s, axis=1, keepdims=True), jnp.max(so, axis=1, keepdims=True)
        )
        w = jnp.exp(s - top)
        wo = jnp.exp(so - top)
        inv = 1.0 / (jnp.sum(w, axis=1, keepdims=True) + jnp.sum(wo, axis=1, keepdims=True))
        o = jnp.dot((w * inv).astype(bf), vals, preferred_element_type=f32)
        return o + jnp.dot((wo * inv).astype(bf), vn, preferred_element_type=f32)

    def slot1(t, piece):
        h, g = divmod(piece, kv_count)
        return heads.at[
            pl.ds(aligned(t * rows + h * GROUP, GROUP), GROUP),
            pl.ds(g * piece_width, piece_width),
        ]

    def along(to, piece, cond):
        here = slot1(tok, piece)
        to = lax.rem(to + 2 * Z, Z)
        start(copy(here, here, a_zs.at[to, piece], a_r.at[tok, piece], t=to * R + r), cond)

    def carry(zs, piece):
        way = jnp.where(zs < z, 1, -1)
        here = slot1(zs * R + r, piece)
        to = lax.rem(z + way + Z, Z)
        start(
            copy(here, here, a_fs.at[zs, piece], a_r.at[zs * R + r, piece], t=to * R + r),
            ((z - zs) * way >= 2) & (z + way >= 0) & (z + way < Z),
        )

    def tell(way):
        pl.semaphore_signal(
            hello.at[(1 - way) // 2],
            inc=1,
            device_id={"tok": tok + way * R, "side": side},
            device_id_type=pl.DeviceIdType.MESH,
        )

    def reach():
        for way in (1, -1):
            to = z + 2 * way
            inside = (to >= 0) & (to < Z)

            @pl.when(inside)
            def _(way=way):
                pl.semaphore_wait(hello.at[(1 + way) // 2], 1)

            for piece in range(pieces):
                along(to, piece, inside)

    def across(zs, piece):
        here = slot1(zs * R + r, piece)
        for e in range(1, R):
            start(
                copy(
                    here,
                    here,
                    a_ys.at[e, zs, piece],
                    a_r.at[zs * R + r, piece],
                    t=z * R + ro(e),
                )
            )

    def landed1(t, piece):
        here = slot1(t, piece)
        copy(here, here, a_r.at[t, piece], a_r.at[t, piece]).wait_recv()

    home = r // RH == side

    for piece in range(pieces):
        h, g = divmod(piece, kv_count)
        for load in kv_loads[piece]:
            load.wait()
        if piece == pieces - 1:
            for load in loads:
                load.start()
        halves = [attend(c, g) for c in range(h * GROUP // CHUNK, (h + 1) * GROUP // CHUNK)]
        at = pl.ds(aligned(tok * rows + h * GROUP, GROUP), GROUP)
        for k in range(group):
            block = jnp.concatenate([o[k * CHUNK : (k + 1) * CHUNK] for o in halves], axis=0)
            col = (g * group + k) * head_width
            heads[at, col : col + head_width] = block.astype(bf)
        if piece == 0:
            pl.semaphore_wait(barrier, neighbours)
            inner = (z > 0) & (z < Z - 1)
            for way in (1, -1):
                pl.when(inner)(functools.partial(tell, way))
        for way in (1, -1):
            along(z + way, piece, (z + way >= 0) & (z + way < Z))
        across(z, piece)

    reach()

    for load in smalls[4:]:
        load.wait()

    for t in range(T):
        hid_out[t] = hidden_ref[:, t * width : (t + 1) * width]

    @pl.when(home)
    def _():
        hid_in[tok] = hid_out[tok]

    def lend(t):
        start(copy(hid_out.at[t], hid_in.at[tok], h_s.at[t], h_r.at[tok], t=t), home)

    for e in range(1, R):
        lend(z * R + ro(e))

    resw[...] = jnp.zeros_like(resw)
    lanes = lax.broadcasted_iota(i32, (1, total), 1)
    block_of = lax.div(lanes, rows)
    route0 = routes_t_ref[0:1, :]
    route1 = routes_t_ref[1:2, :]
    erow = lax.broadcasted_iota(i32, (8, total), 0)
    hit8 = (route0 == erow) | (route1 == erow)
    row_i = lax.broadcasted_iota(i32, (total, total), 0)
    col_i = lax.broadcasted_iota(i32, (total, total), 1)
    before = (row_i < col_i) & (lax.div(row_i, rows) == lax.div(col_i, rows))
    rank8 = jnp.dot(
        jnp.where(hit8, 1.0, 0.0).astype(bf),
        jnp.where(before, 1.0, 0.0).astype(bf),
        preferred_element_type=f32,
    ).astype(i32)
    rank_s[...] = rank8
    zs_of = lax.div(block_of, R)
    place_s[...] = jnp.where(hit8 & (rank8 < cap), lax.rem(zs_of, ZH) * cap + rank8, -1)
    wave_lane_r = lax.rem(
        lax.div(lax.broadcasted_iota(i32, (1, wave_rows), 1), rows), R
    )
    wave_row = lax.broadcasted_iota(i32, (ZH * cap, wave_rows), 0)
    for i, w in enumerate(waves):
        placed = place_s[:, pl.ds(aligned(w * wave_rows, wave_rows), wave_rows)]
        for j in range(RH):
            fits = wave_lane_r == side * RH + j
            for e in range(Z):
                want = jnp.where(fits, placed[e : e + 1], -1)
                put_s[i, j, e * ZH * cap : (e + 1) * ZH * cap, :] = jnp.where(
                    wave_row == want, 1.0, 0.0
                ).astype(bf)
    my_rank = rank_s[pl.ds(z, 1), :]
    my_hit = (route0 == z) | (route1 == z)
    target = jnp.where(
        my_hit & (my_rank < cap),
        (lax.rem(block_of, R) * Z + zs_of) * cap + my_rank,
        -1,
    )
    code = (route0 + route1 - z).astype(f32) + jnp.where(route0 == z, 16.0, 0.0)
    codes = jnp.sum(
        jnp.where(lax.broadcasted_iota(i32, (slots, total), 0) == target, code, 0.0),
        axis=1,
        keepdims=True,
    )
    is_first = jnp.where(codes >= 16.0, 1.0, 0.0)
    first_s[...] = jnp.broadcast_to(is_first, first_s.shape)
    other_s[...] = jnp.broadcast_to((codes - 16.0 * is_first).astype(i32), other_s.shape)

    def xslot(t, rp, w):
        return X.at[t, rp, w]

    def x_across(zs, j, w):
        t, rp = zs * R + r, side * RH + j
        for e in range(1, R):
            start(
                copy(
                    xslot(t, rp, w),
                    xslot(t, rp, w),
                    x_ys.at[e, zs, j, w],
                    x_r.at[t, rp, w],
                    t=z * R + ro(e),
                )
            )

    def x_over(t, j, w):
        rp = side * RH + j
        start(
            copy(
                xslot(t, rp, w), xslot(t, rp, w), x_os.at[t, j, w], x_r.at[t, rp, w], s=other
            )
        )

    def x_landed(t, rp, w):
        copy(xslot(t, rp, w), xslot(t, rp, w), x_r.at[t, rp, w], x_r.at[t, rp, w]).wait_recv()

    def project(i):
        w = waves[i]
        p = jnp.dot(
            heads[pl.ds(aligned(w * wave_rows, wave_rows), wave_rows), :],
            out_w[...],
            preferred_element_type=f32,
        )
        proj[i] = p.reshape(ZH, 2, RH * rows, width)
        c = copy(proj.at[i, :, other], peer.at[i], p_s.at[i], p_r.at[i], s=other)
        start(c)
        for zl in range(ZH):
            for j in range(RH):
                b = (w * ZH + zl) * R + side * RH + j

                @pl.when(b != tok)
                def _(b=b):
                    copy(hid_in.at[b], hid_in.at[b], h_r.at[b], h_r.at[b]).wait_recv()

        c.wait_recv()
        for zl in range(ZH):
            b0 = (w * ZH + zl) * R + side * RH
            whole = (
                proj[i, zl, side]
                + peer[i, zl]
                + hid_in[pl.ds(b0, RH)].astype(f32).reshape(RH * rows, width)
            )
            resw[zl, pl.ds(side * RH, RH)] = whole.astype(bf).reshape(RH, rows, width)
        for j in range(RH):
            packed = jnp.dot(
                put_s[i, j],
                resw[...].reshape(wave_rows, width),
                preferred_element_type=f32,
            )
            stage[i, j] = packed.astype(bf).reshape(Z, ZH * cap, width)
            rp = side * RH + j
            X[tok, rp, w] = stage[i, j, z]
            x_across(z, j, w)
            x_over(tok, j, w)
        for k in range(1, Z):
            deliver(i, k)

    def deliver(i, k):
        zd, w = order[k], waves[i]
        for j in range(RH):
            rp = side * RH + j
            start(
                copy(
                    stage.at[i, j, zd],
                    xslot(tok, rp, w),
                    x_zs.at[i, j, zd],
                    x_r.at[tok, rp, w],
                    t=zd * R + r,
                )
            )

    def relay_z(w, k):
        zs = order[k]
        for j in range(RH):
            x_landed(zs * R + r, side * RH + j, w)
            x_across(zs, j, w)
            x_over(zs * R + r, j, w)

    def relay_y(w, k):
        zs = order[k]
        for e in range(1, R):
            for j in range(RH):
                x_landed(zs * R + ro(e), side * RH + j, w)
                x_over(zs * R + ro(e), j, w)

    loads[0].wait()

    def crossed(zs):
        for e in range(1, R):
            for piece in range(pieces):
                landed1(zs * R + ro(e), piece)

    for k in range(1, Z):
        zs = order[k]
        for piece in range(pieces):
            landed1(zs * R + r, piece)
            if k > 1:
                carry(zs, piece)
            across(zs, piece)
            if piece == 0:
                lend(zs * R + r)
                for e in range(1, R):
                    lend(zs * R + ro(e))
    for w in range(2):
        for zs in range(w * ZH, (w + 1) * ZH):
            crossed(zs)
        project(w)
    tile = min(HIDDEN_TILE, hid)
    strip = half_d // STRIPS

    def spread(block, n):
        return jnp.concatenate([block] * (n // 128), axis=1)

    def absorb(zs, idx, squares, logits):
        for r2 in range(R):
            for rp in range(RH):
                for w in range(2):
                    x_landed(zs * R + r2, other * RH + rp, w)
        x = jnp.concatenate(
            [X[zs * R + r2].reshape(slots, width) for r2 in range(R)], axis=1
        ).astype(f32)
        cols = pl.ds(aligned(zs * wide, wide), wide)
        squares = squares + jnp.sum(x * x, axis=1, keepdims=True)
        a = (x * gain_ref[:, cols]).astype(bf)
        a_s[...] = a
        resid[:, cols] = (x * spread(first_s[...], wide)).astype(bf)
        left = router_ref[:, cols]
        for _ in range(3):
            now = left.astype(bf)
            left = left - now.astype(f32)
            logits = logits + lax.dot_general(
                a, now, (((1,), (1,)), ((), ())), preferred_element_type=f32
            )
        if idx == Z - 1:
            rs = lax.rsqrt(squares / D + 1e-05)
            rs_s[...] = jnp.broadcast_to(rs, rs_s.shape)

        @pl.loop(0, hid // tile)
        def _(n):
            here = pl.ds(aligned(n * tile, tile), tile)
            g = jnp.dot(a_s[...], gate_w[cols, here], preferred_element_type=f32)
            u = jnp.dot(a_s[...], up_w[cols, here], preferred_element_type=f32)
            if idx > 0:
                g = acc_g[:, here] + g
                u = acc_u[:, here] + u
            if idx < Z - 1:
                acc_g[:, here] = g
                acc_u[:, here] = u
            else:
                scale = spread(rs_s[...], tile)
                g = g * scale
                u = u * scale
                active[:, here] = (g / (1.0 + jnp.exp(-g)) * u).astype(bf)

        return squares, logits

    def down(which, q):
        at = pl.ds(aligned(which * half_d + q * strip, 128), strip)
        return jnp.dot(active[...], down_w[:, at], preferred_element_type=f32)

    def y_copy(q, e):
        i = (q, e)
        return copy(y_out.at[i], y_in.at[i], ry_s.at[i], ry_r.at[i], t=z * R + ro(e))

    swaps = []

    def contract(q):
        theirs[q] = down(other, q).astype(bf)
        c = copy(theirs.at[q], theirs_in.at[q], c_s.at[q], c_r.at[q], s=other)
        start(c)
        swaps.append(c)
        mine[q] = down(side, q)

    def pass_on(q):
        swaps[q].wait_recv()
        mine[q] = (mine[q] + theirs_in[q].astype(f32)) * spread(coef_s[...], strip)
        for e in range(1, R):
            at = pl.ds(aligned(ro(e) * part, part), part)
            y_out[q, e] = mine[q, at, :].astype(bf)
            start(y_copy(q, e))

    def send_back(q):
        own = pl.ds(aligned(r * part, part), part)
        cols = pl.ds(aligned(side * half_d + q * strip, 128), strip)
        rows_sum = mine[q, own, :] + resid[own, cols].astype(f32)
        for e in range(1, R):
            y_copy(q, e).wait_recv()
            rows_sum = rows_sum + y_in[q, e].astype(f32)
        for to in range(Z):
            z_out[q, to] = wire(rows_sum[to * cap : (to + 1) * cap])
            c = copy(
                z_out.at[q, to], z_in.at[q, z], rz_s.at[q, to], rz_r.at[q, z], t=to * R + r
            )
            start(c, z != to)

            @pl.when(z == to)
            def _(q=q, to=to):
                z_in[q, z] = z_out[q, to]

    squares, logits = jnp.zeros((slots, 1), f32), jnp.zeros((slots, Z), f32)
    def relay(along_z, k):
        for w in range(2):
            (relay_z if along_z else relay_y)(w, k)

    relay(True, 1)
    relay(False, 0)
    for k in range(Z):
        if k + 2 < Z:
            relay(True, k + 2)
        if k + 1 < Z:
            relay(False, k + 1)
        if k == 0:
            loads[1].wait()
            loads[2].wait()
        squares, logits = absorb(order[k], k, squares, logits)
    logits = logits * rs_s[:, :1]
    elane = lax.broadcasted_iota(i32, (slots, Z), 1)
    l_self = jnp.sum(jnp.where(elane == z, logits, 0.0), axis=1, keepdims=True)
    l_other = jnp.sum(jnp.where(elane == other_s[:, :Z], logits, 0.0), axis=1, keepdims=True)
    coef_s[...] = jnp.broadcast_to(1.0 / (1.0 + jnp.exp(l_other - l_self)), coef_s.shape)
    loads[3].wait()
    for q in range(STRIPS):
        contract(q)
        if q > 0:
            pass_on(q - 1)
    pass_on(STRIPS - 1)

    lane_t = lax.broadcasted_iota(i32, (rows, total), 1)
    at_own = lane_t == tok * rows + lax.broadcasted_iota(i32, (rows, total), 0)
    r0 = jnp.sum(jnp.where(at_own, route0, 0), axis=1, keepdims=True)
    r1 = jnp.sum(jnp.where(at_own, route1, 0), axis=1, keepdims=True)
    lane = lax.broadcasted_iota(i32, (rows, 128), 1)
    both = jnp.where((lane == r0) | (lane == r1), 1.0, 0.0).astype(bf)
    row_n = lax.broadcasted_iota(i32, (rows, rows), 0)
    col_n = lax.broadcasted_iota(i32, (rows, rows), 1)
    ranks = jnp.dot(
        jnp.where(col_n < row_n, 1.0, 0.0).astype(bf), both, preferred_element_type=f32
    ).astype(i32)
    at_part = lax.broadcasted_iota(i32, (rows, part), 1)

    def find(k):
        rank = jnp.sum(jnp.where(lane == k, ranks, 0), axis=1, keepdims=True)
        return at_part == k * cap + rank

    pick = jnp.where(find(r0) | find(r1), 1.0, 0.0).astype(bf)

    for q in range(STRIPS):
        send_back(q)
    for q in range(STRIPS):
        for d in range(1, Z):
            src = lax.rem(z + d, Z)
            here = z_in.at[q, src]
            copy(here, here, rz_r.at[q, src], rz_r.at[q, src]).wait_recv()
        got = jnp.concatenate([unwire(z_in[q, e], strip) for e in range(Z)], axis=0)
        done = jnp.dot(pick, got.astype(bf), preferred_element_type=f32).astype(bf)
        mid = pl.ds(aligned(side * half_d + q * strip, 128), strip)
        out_ref[:, mid] = done
        start(copy(out_ref.at[:, mid], out_ref.at[:, mid], f_s.at[q], f_r.at[q], s=other))
    for q in range(STRIPS):
        mid = pl.ds(aligned(other * half_d + q * strip, 128), strip)
        copy(out_ref.at[:, mid], out_ref.at[:, mid], f_r.at[q], f_r.at[q]).wait_recv()
    for c, cond in pending:
        if cond is None:
            c.wait_send()
        else:
            pl.when(cond)(c.wait_send)


def local(
    hidden_in,
    queries,
    key_new,
    value_new,
    cache_keys,
    cache_values,
    lengths,
    out_weight,
    norm_gain,
    router_weight,
    gate_weight,
    up_weight,
    down_weight,
    routes,
):
    rows, D = hidden_in.shape
    _, head_count, head_width = queries.shape
    kv_count = key_new.shape[1]
    T = lax.axis_size("tok")
    Z = router_weight.shape[1]
    R = T // Z
    ZH, RH = Z // 2, R // 2
    cap = min(CAP, rows)
    slots = T * cap
    part = Z * cap
    hid = gate_weight.shape[1]
    width = out_weight.shape[1]
    wave_rows = ZH * R * rows
    pieces = (rows // GROUP) * kv_count
    half_d = D // 2
    strip = half_d // STRIPS
    wire_width = strip * cap // 16
    dma = pltpu.SemaphoreType.DMA
    vmem = pl.BlockSpec(memory_space=pltpu.VMEM)
    anyspace = pl.BlockSpec(memory_space=pl.ANY)
    return pl.pallas_call(
        functools.partial(body, (T, Z, R, rows, cap)),
        out_shape=pltpu.VMEM((rows, D), bf),
        in_specs=[anyspace] * 14,
        out_specs=vmem,
        scratch_shapes=[
            pltpu.VMEM((1, rows), i32),
            pltpu.VMEM((head_count, rows, head_width), bf),
            pltpu.VMEM((rows * kv_count, head_width), bf),
            pltpu.VMEM((rows * kv_count, head_width), bf),
            pltpu.VMEM((rows, D), bf),
            pltpu.VMEM((2, T * rows), i32),
            pltpu.VMEM((1, D), f32),
            pltpu.VMEM((Z, D), f32),
            dma((8,)),
            pltpu.VMEM(cache_keys.shape, bf),
            pltpu.VMEM(cache_values.shape, bf),
            pltpu.VMEM((T * rows, head_count * head_width), bf),
            pltpu.VMEM((T, rows, width), bf),
            pltpu.VMEM((T, rows, width), bf),
            pltpu.VMEM((2, ZH, 2, RH * rows, width), f32),
            pltpu.VMEM((2, ZH, RH * rows, width), f32),
            pltpu.VMEM((ZH, R, rows, width), bf),
            pltpu.VMEM((8, T * rows), i32),
            pltpu.VMEM((8, T * rows), i32),
            pltpu.VMEM((2, RH, Z * ZH * cap, wave_rows), bf),
            pltpu.VMEM((2, RH, Z, ZH * cap, width), bf),
            pltpu.VMEM((T, R, 2, ZH * cap, width), bf),
            pltpu.VMEM((slots, 128), f32),
            pltpu.VMEM((slots, 128), i32),
            pltpu.VMEM((slots, 128), f32),
            pltpu.VMEM((slots, 128), f32),
            pltpu.VMEM((slots, D), bf),
            pltpu.VMEM((slots, R * width), bf),
            pltpu.VMEM((slots, hid), f32),
            pltpu.VMEM((slots, hid), f32),
            pltpu.VMEM((slots, hid), bf),
            pltpu.VMEM(out_weight.shape, bf),
            pltpu.VMEM(gate_weight.shape, bf),
            pltpu.VMEM(up_weight.shape, bf),
            pltpu.VMEM(down_weight.shape, bf),
            pltpu.VMEM((STRIPS, slots, strip), f32),
            pltpu.VMEM((STRIPS, slots, strip), bf),
            pltpu.VMEM((STRIPS, slots, strip), bf),
            pltpu.VMEM((STRIPS, R, part, strip), bf),
            pltpu.VMEM((STRIPS, R, part, strip), bf),
            pltpu.VMEM((STRIPS, Z, 16, wire_width), bf),
            pltpu.VMEM((STRIPS, Z, 16, wire_width), bf),
            dma((2, pieces)),
            dma((4,)),
            pltpu.SemaphoreType.REGULAR((2,)),
            dma((Z, pieces)),
            dma((Z, pieces)),
            dma((R, Z, pieces)),
            dma((T, pieces)),
            dma((T,)),
            dma((T,)),
            dma((2,)),
            dma((2,)),
            dma((2, RH, Z)),
            dma((R, Z, RH, 2)),
            dma((T, RH, 2)),
            dma((T, R, 2)),
            dma((STRIPS,)),
            dma((STRIPS,)),
            dma((STRIPS, R)),
            dma((STRIPS, R)),
            dma((STRIPS, Z)),
            dma((STRIPS, Z)),
            dma((STRIPS,)),
            dma((STRIPS,)),
        ],
        compiler_params=pltpu.CompilerParams(
            collective_id=0, has_side_effects=True, vmem_limit_bytes=66600000
        ),
    )(
        lengths.reshape(1, rows),
        jnp.transpose(queries, (1, 0, 2)),
        key_new.reshape(rows * kv_count, head_width),
        value_new.reshape(rows * kv_count, head_width),
        hidden_in,
        routes.T,
        norm_gain.reshape(1, D),
        router_weight.T,
        cache_keys,
        cache_values,
        out_weight,
        gate_weight,
        up_weight,
        down_weight,
    )


def solution(mesh):
    return jax.shard_map(
        local,
        mesh=mesh,
        in_specs=(
            P(("grp", "tok"), None),
            P(("grp", "tok"), "side", None),
            P(("grp", "tok"), "side", None),
            P(("grp", "tok"), "side", None),
            P(("grp", "tok"), "side", None, None),
            P(("grp", "tok"), "side", None, None),
            P(("grp", "tok")),
            P("side", "tok"),
            P(),
            P(),
            P(None, ("tok", "side")),
            P(None, ("tok", "side")),
            P(("tok", "side"), None),
            P("grp", None),
        ),
        out_specs=P(("grp", "tok"), None),
        check_vma=False,
    )
```

```python
import functools
import math

import jax
import jax.numpy as jnp
from jax import lax
from jax.experimental import pallas as pl
from jax.experimental.pallas import tpu as pltpu
from jax.sharding import PartitionSpec as P

CAP = 24
HIDDEN_TILE = 2048
STRIPS = 3
GROUP = 16
CHUNK = 8

bf, f32, i32 = jnp.bfloat16, jnp.float32, jnp.int32


def wire(block):
    rows, width = block.shape
    half = width // 2
    tail = jnp.concatenate([block[16:, :half], block[16:, half:]], axis=0)
    return jnp.concatenate([block[:16], tail], axis=1).astype(bf)


def unwire(block, width):
    half = width // 2
    full = block.astype(f32)
    tail = jnp.concatenate([full[:8, width:], full[8:, width:]], axis=1)
    return jnp.concatenate([full[:, :width], tail], axis=0)


def aligned(start, step):
    return pl.multiple_of(start, step)


def body(
    dims,
    lengths_hbm,
    q_hbm,
    kn_hbm,
    vn_hbm,
    hidden_hbm,
    routes_t_hbm,
    gain_hbm,
    router_hbm,
    k_hbm,
    v_hbm,
    out_hbm,
    gate_hbm,
    up_hbm,
    down_hbm,
    out_ref,
    lengths_ref,
    q_ref,
    kn_ref,
    vn_ref,
    hidden_ref,
    routes_t_ref,
    gain_ref,
    router_ref,
    small_sem,
    k_buf,
    v_buf,
    heads,
    hid_out,
    hid_in,
    proj,
    peer,
    resw,
    place_s,
    rank_s,
    put_s,
    stage,
    X,
    first_s,
    other_s,
    rs_s,
    coef_s,
    resid,
    a_s,
    acc_g,
    acc_u,
    active,
    out_w,
    gate_w,
    up_w,
    down_w,
    mine,
    theirs,
    theirs_in,
    y_out,
    y_in,
    z_out,
    z_in,
    kv_sem,
    w_sem,
    hello,
    a_zs,
    a_fs,
    a_ys,
    a_r,
    h_s,
    h_r,
    p_s,
    p_r,
    x_zs,
    x_ys,
    x_os,
    x_r,
    c_s,
    c_r,
    ry_s,
    ry_r,
    rz_s,
    rz_r,
    f_s,
    f_r,
):
    T, Z, R, rows, cap = dims
    ZH, RH = Z // 2, R // 2
    D = hidden_ref.shape[1]
    half_d = D // 2
    total = T * rows
    slots = T * cap
    part = Z * cap
    hid = gate_w.shape[1]
    width = out_w.shape[1]
    wide = R * width
    wave_rows = ZH * R * rows
    _, kv_count, places, head_width = k_buf.shape
    group = q_ref.shape[0] // kv_count
    pieces = (rows // GROUP) * kv_count
    piece_width = group * head_width
    tok = lax.axis_index("tok")
    side = lax.axis_index("side")
    z = tok // R
    r = tok % R
    other = 1 - side
    def ro(d):
        return (r + d) % R

    order = [jnp.where(k <= z, z - k, k) for k in range(Z)]
    top_chip = jnp.where(z == Z - 1, 1, 0)
    waves = [top_chip, 1 - top_chip]

    def copy(src, dst, ssem, rsem, t=None, s=None):
        where = {"tok": tok if t is None else t, "side": side if s is None else s}
        return pltpu.make_async_remote_copy(
            src_ref=src,
            dst_ref=dst,
            send_sem=ssem,
            recv_sem=rsem,
            device_id=where,
            device_id_type=pl.DeviceIdType.MESH,
        )

    pending = []

    def start(c, cond=None):
        pending.append((c, cond))
        if cond is None:
            c.start()
        else:
            pl.when(cond)(c.start)

    def drain(copies):
        for c, cond in copies:
            if cond is None:
                c.wait_send()
            else:
                pl.when(cond)(c.wait_send)

    barrier = pltpu.get_barrier_semaphore()

    def greet(t, s):
        pl.semaphore_signal(
            barrier,
            inc=1,
            device_id={"tok": t, "side": s},
            device_id_type=pl.DeviceIdType.MESH,
        )

    @pl.when(z > 0)
    def _():
        greet(tok - R, side)

    @pl.when(z < Z - 1)
    def _():
        greet(tok + R, side)

    for e in range(1, R):
        greet(z * R + ro(e), side)
    greet(tok, other)
    neighbours = R + jnp.where(z > 0, 1, 0) + jnp.where(z < Z - 1, 1, 0)

    def kv_load(piece):
        h, g = divmod(piece, kv_count)
        at = pl.ds(h * GROUP, GROUP)
        return [
            pltpu.make_async_copy(k_hbm.at[at, g], k_buf.at[at, g], kv_sem.at[0, piece]),
            pltpu.make_async_copy(v_hbm.at[at, g], v_buf.at[at, g], kv_sem.at[1, piece]),
        ]

    smalls = [
        pltpu.make_async_copy(src, dst, small_sem.at[i])
        for i, (src, dst) in enumerate(
            (
                (lengths_hbm, lengths_ref),
                (q_hbm, q_ref),
                (kn_hbm, kn_ref),
                (vn_hbm, vn_ref),
                (hidden_hbm, hidden_ref),
                (routes_t_hbm, routes_t_ref),
                (gain_hbm, gain_ref),
                (router_hbm, router_ref),
            )
        )
    ]
    for load in smalls[:4]:
        load.start()
    kv_loads = [kv_load(piece) for piece in range(pieces)]
    for pair in kv_loads:
        for load in pair:
            load.start()
    for load in smalls[4:]:
        load.start()
    for load in smalls[:4]:
        load.wait()
    loads = [
        pltpu.make_async_copy(out_hbm, out_w, w_sem.at[0]),
        pltpu.make_async_copy(gate_hbm, gate_w, w_sem.at[1]),
        pltpu.make_async_copy(up_hbm, up_w, w_sem.at[2]),
        pltpu.make_async_copy(down_hbm, down_w, w_sem.at[3]),
    ]

    scaling = 1.0 / math.sqrt(head_width)
    eye = lax.broadcasted_iota(i32, (rows, rows), 0) == lax.broadcasted_iota(i32, (rows, rows), 1)
    lens = jnp.sum(jnp.where(eye, lengths_ref[...], 0), axis=1, keepdims=True)
    unit = group * CHUNK
    seq_of = lax.rem(lax.broadcasted_iota(i32, (unit, 1), 0), CHUNK)
    cols_at = lax.broadcasted_iota(i32, (unit, CHUNK * places), 1) - seq_of * places
    own_at = lax.broadcasted_iota(i32, (unit, rows * kv_count), 1) - seq_of * kv_count
    low = -1e30
    kn = kn_ref[...]
    vn = vn_ref[...]

    def attend(c, g):
        q = q_ref[g * group : (g + 1) * group, c * CHUNK : (c + 1) * CHUNK, :]
        q = q.astype(f32).reshape(unit, head_width).astype(bf)
        keys = k_buf[c * CHUNK : (c + 1) * CHUNK, g].reshape(CHUNK * places, head_width)
        vals = v_buf[c * CHUNK : (c + 1) * CHUNK, g].reshape(CHUNK * places, head_width)
        dn = (((1,), (1,)), ((), ()))
        s = lax.dot_general(q, keys, dn, preferred_element_type=f32) * scaling
        so = lax.dot_general(q, kn, dn, preferred_element_type=f32) * scaling
        size = jnp.concatenate([lens[c * CHUNK : (c + 1) * CHUNK]] * group, axis=0)
        s = jnp.where((cols_at >= 0) & (cols_at < size), s, low)
        so = jnp.where(own_at == c * CHUNK * kv_count + g, so, low)
        top = jnp.maximum(
            jnp.max(s, axis=1, keepdims=True), jnp.max(so, axis=1, keepdims=True)
        )
        w = jnp.exp(s - top)
        wo = jnp.exp(so - top)
        inv = 1.0 / (jnp.sum(w, axis=1, keepdims=True) + jnp.sum(wo, axis=1, keepdims=True))
        o = jnp.dot((w * inv).astype(bf), vals, preferred_element_type=f32)
        return o + jnp.dot((wo * inv).astype(bf), vn, preferred_element_type=f32)

    def slot1(t, piece):
        h, g = divmod(piece, kv_count)
        return heads.at[
            pl.ds(aligned(t * rows + h * GROUP, GROUP), GROUP),
            pl.ds(g * piece_width, piece_width),
        ]

    def along(to, piece, cond):
        here = slot1(tok, piece)
        to = lax.rem(to + 2 * Z, Z)
        start(copy(here, here, a_zs.at[to, piece], a_r.at[tok, piece], t=to * R + r), cond)

    def carry(zs, piece):
        way = jnp.where(zs < z, 1, -1)
        here = slot1(zs * R + r, piece)
        to = lax.rem(z + way + Z, Z)
        start(
            copy(here, here, a_fs.at[zs, piece], a_r.at[zs * R + r, piece], t=to * R + r),
            ((z - zs) * way >= 2) & (z + way >= 0) & (z + way < Z),
        )

    def tell(way):
        pl.semaphore_signal(
            hello.at[(1 - way) // 2],
            inc=1,
            device_id={"tok": tok + way * R, "side": side},
            device_id_type=pl.DeviceIdType.MESH,
        )

    def meet():
        for way in (1, -1):

            @pl.when((z + 2 * way >= 0) & (z + 2 * way < Z))
            def _(way=way):
                pl.semaphore_wait(hello.at[(1 + way) // 2], 1)

    def reach(piece):
        for way in (1, -1):
            to = z + 2 * way
            along(to, piece, (to >= 0) & (to < Z))

    def across(zs, piece):
        here = slot1(zs * R + r, piece)
        for e in range(1, R):
            start(
                copy(
                    here,
                    here,
                    a_ys.at[e, zs, piece],
                    a_r.at[zs * R + r, piece],
                    t=z * R + ro(e),
                )
            )

    def landed1(t, piece):
        here = slot1(t, piece)
        copy(here, here, a_r.at[t, piece], a_r.at[t, piece]).wait_recv()

    home = r // RH == side

    for piece in range(pieces):
        h, g = divmod(piece, kv_count)
        for load in kv_loads[piece]:
            load.wait()
        if piece == pieces - 1:
            for load in loads:
                load.start()
        halves = [attend(c, g) for c in range(h * GROUP // CHUNK, (h + 1) * GROUP // CHUNK)]
        at = pl.ds(aligned(tok * rows + h * GROUP, GROUP), GROUP)
        for k in range(group):
            block = jnp.concatenate([o[k * CHUNK : (k + 1) * CHUNK] for o in halves], axis=0)
            col = (g * group + k) * head_width
            heads[at, col : col + head_width] = block.astype(bf)
        if piece == 0:
            pl.semaphore_wait(barrier, neighbours)
            inner = (z > 0) & (z < Z - 1)
            for way in (1, -1):
                pl.when(inner)(functools.partial(tell, way))
        for way in (1, -1):
            along(z + way, piece, (z + way >= 0) & (z + way < Z))
        across(z, piece)
        if piece == pieces - 2:
            meet()
            for earlier in range(piece):
                reach(earlier)
        if piece >= pieces - 2:
            reach(piece)

    for load in smalls[4:]:
        load.wait()

    for t in range(T):
        hid_out[t] = hidden_ref[:, t * width : (t + 1) * width]

    @pl.when(home)
    def _():
        hid_in[tok] = hid_out[tok]

    def lend(t):
        start(copy(hid_out.at[t], hid_in.at[tok], h_s.at[t], h_r.at[tok], t=t), home)

    for e in range(1, R):
        lend(z * R + ro(e))

    resw[...] = jnp.zeros_like(resw)
    lanes = lax.broadcasted_iota(i32, (1, total), 1)
    block_of = lax.div(lanes, rows)
    route0 = routes_t_ref[0:1, :]
    route1 = routes_t_ref[1:2, :]
    erow = lax.broadcasted_iota(i32, (8, total), 0)
    hit8 = (route0 == erow) | (route1 == erow)
    row_i = lax.broadcasted_iota(i32, (total, total), 0)
    col_i = lax.broadcasted_iota(i32, (total, total), 1)
    before = (row_i < col_i) & (lax.div(row_i, rows) == lax.div(col_i, rows))
    rank8 = jnp.dot(
        jnp.where(hit8, 1.0, 0.0).astype(bf),
        jnp.where(before, 1.0, 0.0).astype(bf),
        preferred_element_type=f32,
    ).astype(i32)
    rank_s[...] = rank8
    zs_of = lax.div(block_of, R)
    place_s[...] = jnp.where(hit8 & (rank8 < cap), lax.rem(zs_of, ZH) * cap + rank8, -1)
    wave_lane_r = lax.rem(
        lax.div(lax.broadcasted_iota(i32, (1, wave_rows), 1), rows), R
    )
    wave_row = lax.broadcasted_iota(i32, (ZH * cap, wave_rows), 0)
    for i, w in enumerate(waves):
        placed = place_s[:, pl.ds(aligned(w * wave_rows, wave_rows), wave_rows)]
        for j in range(RH):
            fits = wave_lane_r == side * RH + j
            for e in range(Z):
                want = jnp.where(fits, placed[e : e + 1], -1)
                put_s[i, j, e * ZH * cap : (e + 1) * ZH * cap, :] = jnp.where(
                    wave_row == want, 1.0, 0.0
                ).astype(bf)
    my_rank = rank_s[pl.ds(z, 1), :]
    my_hit = (route0 == z) | (route1 == z)
    target = jnp.where(
        my_hit & (my_rank < cap),
        (lax.rem(block_of, R) * Z + zs_of) * cap + my_rank,
        -1,
    )
    code = (route0 + route1 - z).astype(f32) + jnp.where(route0 == z, 16.0, 0.0)
    codes = jnp.sum(
        jnp.where(lax.broadcasted_iota(i32, (slots, total), 0) == target, code, 0.0),
        axis=1,
        keepdims=True,
    )
    is_first = jnp.where(codes >= 16.0, 1.0, 0.0)
    first_s[...] = jnp.broadcast_to(is_first, first_s.shape)
    other_s[...] = jnp.broadcast_to((codes - 16.0 * is_first).astype(i32), other_s.shape)

    def xslot(t, rp, w):
        return X.at[t, rp, w]

    def x_across(zs, j, w):
        t, rp = zs * R + r, side * RH + j
        for e in range(1, R):
            start(
                copy(
                    xslot(t, rp, w),
                    xslot(t, rp, w),
                    x_ys.at[e, zs, j, w],
                    x_r.at[t, rp, w],
                    t=z * R + ro(e),
                )
            )

    def x_over(t, j, w):
        rp = side * RH + j
        start(
            copy(
                xslot(t, rp, w), xslot(t, rp, w), x_os.at[t, j, w], x_r.at[t, rp, w], s=other
            )
        )

    def x_landed(t, rp, w):
        copy(xslot(t, rp, w), xslot(t, rp, w), x_r.at[t, rp, w], x_r.at[t, rp, w]).wait_recv()

    def project(i):
        w = waves[i]
        p = jnp.dot(
            heads[pl.ds(aligned(w * wave_rows, wave_rows), wave_rows), :],
            out_w[...],
            preferred_element_type=f32,
        )
        proj[i] = p.reshape(ZH, 2, RH * rows, width)
        c = copy(proj.at[i, :, other], peer.at[i], p_s.at[i], p_r.at[i], s=other)
        start(c)
        for zl in range(ZH):
            for j in range(RH):
                b = (w * ZH + zl) * R + side * RH + j

                @pl.when(b != tok)
                def _(b=b):
                    copy(hid_in.at[b], hid_in.at[b], h_r.at[b], h_r.at[b]).wait_recv()

        c.wait_recv()
        for zl in range(ZH):
            b0 = (w * ZH + zl) * R + side * RH
            whole = (
                proj[i, zl, side]
                + peer[i, zl]
                + hid_in[pl.ds(b0, RH)].astype(f32).reshape(RH * rows, width)
            )
            resw[zl, pl.ds(side * RH, RH)] = whole.astype(bf).reshape(RH, rows, width)
        for j in range(RH):
            packed = jnp.dot(
                put_s[i, j],
                resw[...].reshape(wave_rows, width),
                preferred_element_type=f32,
            )
            stage[i, j] = packed.astype(bf).reshape(Z, ZH * cap, width)
            rp = side * RH + j
            X[tok, rp, w] = stage[i, j, z]
            x_across(z, j, w)
            x_over(tok, j, w)
        for k in range(1, Z):
            deliver(i, k)

    def deliver(i, k):
        zd, w = order[k], waves[i]
        for j in range(RH):
            rp = side * RH + j
            start(
                copy(
                    stage.at[i, j, zd],
                    xslot(tok, rp, w),
                    x_zs.at[i, j, zd],
                    x_r.at[tok, rp, w],
                    t=zd * R + r,
                )
            )

    def relay_z(w, k):
        zs = order[k]
        for j in range(RH):
            x_landed(zs * R + r, side * RH + j, w)
            x_across(zs, j, w)
            x_over(zs * R + r, j, w)

    def relay_y(w, k):
        zs = order[k]
        for e in range(1, R):
            for j in range(RH):
                x_landed(zs * R + ro(e), side * RH + j, w)
                x_over(zs * R + ro(e), j, w)

    loads[0].wait()

    def crossed(zs):
        for e in range(1, R):
            for piece in range(pieces):
                landed1(zs * R + ro(e), piece)

    for k in range(1, Z):
        zs = order[k]
        for piece in range(pieces):
            landed1(zs * R + r, piece)
            if k > 1:
                carry(zs, piece)
            across(zs, piece)
            if piece == 0:
                lend(zs * R + r)
                for e in range(1, R):
                    lend(zs * R + ro(e))
    for i, w in enumerate(waves):
        for zl in range(ZH):
            crossed(w * ZH + zl)
        project(i)
    tile = min(HIDDEN_TILE, hid)
    strip = half_d // STRIPS

    def spread(block, n):
        return jnp.concatenate([block] * (n // 128), axis=1)

    def absorb(zs, idx, squares, logits):
        for r2 in range(R):
            for rp in range(RH):
                for w in range(2):
                    x_landed(zs * R + r2, other * RH + rp, w)
        x = jnp.concatenate(
            [X[zs * R + r2].reshape(slots, width) for r2 in range(R)], axis=1
        ).astype(f32)
        cols = pl.ds(aligned(zs * wide, wide), wide)
        squares = squares + jnp.sum(x * x, axis=1, keepdims=True)
        a = (x * gain_ref[:, cols]).astype(bf)
        a_s[...] = a
        resid[:, cols] = (x * spread(first_s[...], wide)).astype(bf)
        left = router_ref[:, cols]
        for _ in range(3):
            now = left.astype(bf)
            left = left - now.astype(f32)
            logits = logits + lax.dot_general(
                a, now, (((1,), (1,)), ((), ())), preferred_element_type=f32
            )
        if idx == Z - 1:
            rs = lax.rsqrt(squares / D + 1e-05)
            rs_s[...] = jnp.broadcast_to(rs, rs_s.shape)

        @pl.loop(0, hid // tile)
        def _(n):
            here = pl.ds(aligned(n * tile, tile), tile)
            g = jnp.dot(a_s[...], gate_w[cols, here], preferred_element_type=f32)
            u = jnp.dot(a_s[...], up_w[cols, here], preferred_element_type=f32)
            if idx > 0:
                g = acc_g[:, here] + g
                u = acc_u[:, here] + u
            if idx < Z - 1:
                acc_g[:, here] = g
                acc_u[:, here] = u
            else:
                scale = spread(rs_s[...], tile)
                g = g * scale
                u = u * scale
                active[:, here] = (g / (1.0 + jnp.exp(-g)) * u).astype(bf)

        return squares, logits

    def down(which, q):
        at = pl.ds(aligned(which * half_d + q * strip, 128), strip)
        return jnp.dot(active[...], down_w[:, at], preferred_element_type=f32)

    def y_copy(q, e):
        i = (q, e)
        return copy(y_out.at[i], y_in.at[i], ry_s.at[i], ry_r.at[i], t=z * R + ro(e))

    swaps = []

    def contract(q):
        theirs[q] = down(other, q).astype(bf)
        c = copy(theirs.at[q], theirs_in.at[q], c_s.at[q], c_r.at[q], s=other)
        start(c)
        swaps.append(c)
        if q > 0:
            pass_on(q - 1)
        mine[q] = down(side, q)

    def pass_on(q):
        swaps[q].wait_recv()
        mine[q] = (mine[q] + theirs_in[q].astype(f32)) * spread(coef_s[...], strip)
        for e in range(1, R):
            at = pl.ds(aligned(ro(e) * part, part), part)
            y_out[q, e] = mine[q, at, :].astype(bf)
            start(y_copy(q, e))

    def send_back(q):
        own = pl.ds(aligned(r * part, part), part)
        cols = pl.ds(aligned(side * half_d + q * strip, 128), strip)
        rows_sum = mine[q, own, :] + resid[own, cols].astype(f32)
        for e in range(1, R):
            y_copy(q, e).wait_recv()
            rows_sum = rows_sum + y_in[q, e].astype(f32)
        for to in range(Z):
            z_out[q, to] = wire(rows_sum[to * cap : (to + 1) * cap])
            c = copy(
                z_out.at[q, to], z_in.at[q, z], rz_s.at[q, to], rz_r.at[q, z], t=to * R + r
            )
            start(c, z != to)

            @pl.when(z == to)
            def _(q=q, to=to):
                z_in[q, z] = z_out[q, to]

    squares, logits = jnp.zeros((slots, 1), f32), jnp.zeros((slots, Z), f32)
    def relay(along_z, k):
        for w in range(2):
            (relay_z if along_z else relay_y)(w, k)

    relay(True, 1)
    relay(False, 0)
    for k in range(Z):
        if k + 2 < Z:
            relay(True, k + 2)
        if k + 1 < Z:
            relay(False, k + 1)
        if k == 0:
            loads[1].wait()
            loads[2].wait()
        squares, logits = absorb(order[k], k, squares, logits)
    logits = logits * rs_s[:, :1]
    elane = lax.broadcasted_iota(i32, (slots, Z), 1)
    l_self = jnp.sum(jnp.where(elane == z, logits, 0.0), axis=1, keepdims=True)
    l_other = jnp.sum(jnp.where(elane == other_s[:, :Z], logits, 0.0), axis=1, keepdims=True)
    coef_s[...] = jnp.broadcast_to(1.0 / (1.0 + jnp.exp(l_other - l_self)), coef_s.shape)
    loads[3].wait()
    settled = len(pending)
    for q in range(STRIPS):
        contract(q)
    pass_on(STRIPS - 1)

    lane_t = lax.broadcasted_iota(i32, (rows, total), 1)
    at_own = lane_t == tok * rows + lax.broadcasted_iota(i32, (rows, total), 0)
    r0 = jnp.sum(jnp.where(at_own, route0, 0), axis=1, keepdims=True)
    r1 = jnp.sum(jnp.where(at_own, route1, 0), axis=1, keepdims=True)
    lane = lax.broadcasted_iota(i32, (rows, 128), 1)
    both = jnp.where((lane == r0) | (lane == r1), 1.0, 0.0).astype(bf)
    row_n = lax.broadcasted_iota(i32, (rows, rows), 0)
    col_n = lax.broadcasted_iota(i32, (rows, rows), 1)
    ranks = jnp.dot(
        jnp.where(col_n < row_n, 1.0, 0.0).astype(bf), both, preferred_element_type=f32
    ).astype(i32)
    at_part = lax.broadcasted_iota(i32, (rows, part), 1)

    def find(k):
        rank = jnp.sum(jnp.where(lane == k, ranks, 0), axis=1, keepdims=True)
        return at_part == k * cap + rank

    pick = jnp.where(find(r0) | find(r1), 1.0, 0.0).astype(bf)

    drain(pending[:settled])
    for q in range(STRIPS):
        send_back(q)
    for q in range(STRIPS):
        for d in range(1, Z):
            src = lax.rem(z + d, Z)
            here = z_in.at[q, src]
            copy(here, here, rz_r.at[q, src], rz_r.at[q, src]).wait_recv()
        got = jnp.concatenate([unwire(z_in[q, e], strip) for e in range(Z)], axis=0)
        done = jnp.dot(pick, got.astype(bf), preferred_element_type=f32).astype(bf)
        mid = pl.ds(aligned(side * half_d + q * strip, 128), strip)
        out_ref[:, mid] = done
        start(copy(out_ref.at[:, mid], out_ref.at[:, mid], f_s.at[q], f_r.at[q], s=other))
    for q in range(STRIPS):
        mid = pl.ds(aligned(other * half_d + q * strip, 128), strip)
        copy(out_ref.at[:, mid], out_ref.at[:, mid], f_r.at[q], f_r.at[q]).wait_recv()
    drain(pending[settled:])


def local(
    hidden_in,
    queries,
    key_new,
    value_new,
    cache_keys,
    cache_values,
    lengths,
    out_weight,
    norm_gain,
    router_weight,
    gate_weight,
    up_weight,
    down_weight,
    routes,
):
    rows, D = hidden_in.shape
    _, head_count, head_width = queries.shape
    kv_count = key_new.shape[1]
    T = lax.axis_size("tok")
    Z = router_weight.shape[1]
    R = T // Z
    ZH, RH = Z // 2, R // 2
    cap = min(CAP, rows)
    slots = T * cap
    part = Z * cap
    hid = gate_weight.shape[1]
    width = out_weight.shape[1]
    wave_rows = ZH * R * rows
    pieces = (rows // GROUP) * kv_count
    half_d = D // 2
    strip = half_d // STRIPS
    wire_width = strip * cap // 16
    dma = pltpu.SemaphoreType.DMA
    vmem = pl.BlockSpec(memory_space=pltpu.VMEM)
    anyspace = pl.BlockSpec(memory_space=pl.ANY)
    return pl.pallas_call(
        functools.partial(body, (T, Z, R, rows, cap)),
        out_shape=pltpu.VMEM((rows, D), bf),
        in_specs=[anyspace] * 14,
        out_specs=vmem,
        scratch_shapes=[
            pltpu.VMEM((1, rows), i32),
            pltpu.VMEM((head_count, rows, head_width), bf),
            pltpu.VMEM((rows * kv_count, head_width), bf),
            pltpu.VMEM((rows * kv_count, head_width), bf),
            pltpu.VMEM((rows, D), bf),
            pltpu.VMEM((2, T * rows), i32),
            pltpu.VMEM((1, D), f32),
            pltpu.VMEM((Z, D), f32),
            dma((8,)),
            pltpu.VMEM(cache_keys.shape, bf),
            pltpu.VMEM(cache_values.shape, bf),
            pltpu.VMEM((T * rows, head_count * head_width), bf),
            pltpu.VMEM((T, rows, width), bf),
            pltpu.VMEM((T, rows, width), bf),
            pltpu.VMEM((2, ZH, 2, RH * rows, width), f32),
            pltpu.VMEM((2, ZH, RH * rows, width), f32),
            pltpu.VMEM((ZH, R, rows, width), bf),
            pltpu.VMEM((8, T * rows), i32),
            pltpu.VMEM((8, T * rows), i32),
            pltpu.VMEM((2, RH, Z * ZH * cap, wave_rows), bf),
            pltpu.VMEM((2, RH, Z, ZH * cap, width), bf),
            pltpu.VMEM((T, R, 2, ZH * cap, width), bf),
            pltpu.VMEM((slots, 128), f32),
            pltpu.VMEM((slots, 128), i32),
            pltpu.VMEM((slots, 128), f32),
            pltpu.VMEM((slots, 128), f32),
            pltpu.VMEM((slots, D), bf),
            pltpu.VMEM((slots, R * width), bf),
            pltpu.VMEM((slots, hid), f32),
            pltpu.VMEM((slots, hid), f32),
            pltpu.VMEM((slots, hid), bf),
            pltpu.VMEM(out_weight.shape, bf),
            pltpu.VMEM(gate_weight.shape, bf),
            pltpu.VMEM(up_weight.shape, bf),
            pltpu.VMEM(down_weight.shape, bf),
            pltpu.VMEM((STRIPS, slots, strip), f32),
            pltpu.VMEM((STRIPS, slots, strip), bf),
            pltpu.VMEM((STRIPS, slots, strip), bf),
            pltpu.VMEM((STRIPS, R, part, strip), bf),
            pltpu.VMEM((STRIPS, R, part, strip), bf),
            pltpu.VMEM((STRIPS, Z, 16, wire_width), bf),
            pltpu.VMEM((STRIPS, Z, 16, wire_width), bf),
            dma((2, pieces)),
            dma((4,)),
            pltpu.SemaphoreType.REGULAR((2,)),
            dma((Z, pieces)),
            dma((Z, pieces)),
            dma((R, Z, pieces)),
            dma((T, pieces)),
            dma((T,)),
            dma((T,)),
            dma((2,)),
            dma((2,)),
            dma((2, RH, Z)),
            dma((R, Z, RH, 2)),
            dma((T, RH, 2)),
            dma((T, R, 2)),
            dma((STRIPS,)),
            dma((STRIPS,)),
            dma((STRIPS, R)),
            dma((STRIPS, R)),
            dma((STRIPS, Z)),
            dma((STRIPS, Z)),
            dma((STRIPS,)),
            dma((STRIPS,)),
        ],
        compiler_params=pltpu.CompilerParams(
            collective_id=0, has_side_effects=True, vmem_limit_bytes=66600000
        ),
    )(
        lengths.reshape(1, rows),
        jnp.transpose(queries, (1, 0, 2)),
        key_new.reshape(rows * kv_count, head_width),
        value_new.reshape(rows * kv_count, head_width),
        hidden_in,
        routes.T,
        norm_gain.reshape(1, D),
        router_weight.T,
        cache_keys,
        cache_values,
        out_weight,
        gate_weight,
        up_weight,
        down_weight,
    )


def solution(mesh):
    return jax.shard_map(
        local,
        mesh=mesh,
        in_specs=(
            P(("grp", "tok"), None),
            P(("grp", "tok"), "side", None),
            P(("grp", "tok"), "side", None),
            P(("grp", "tok"), "side", None),
            P(("grp", "tok"), "side", None, None),
            P(("grp", "tok"), "side", None, None),
            P(("grp", "tok")),
            P("side", "tok"),
            P(),
            P(),
            P(None, ("tok", "side")),
            P(None, ("tok", "side")),
            P(("tok", "side"), None),
            P("grp", None),
        ),
        out_specs=P(("grp", "tok"), None),
        check_vma=False,
    )
```
